32 devices in a mesh: model: 4 (over z), sub: 2 (over y), data: 4 (over x, core).
Axes of the slice: x: 2, y: 2, z: 4, core: 2. Of those that a mesh axis runs over, the one named last changes fastest.
Arguments:
- images: bfloat16 [256, 196, 512], P(('model', 'sub', 'data'))
- targets: bfloat16 [256, 196, 512], P(('model', 'sub', 'data'))
- w_in: float32 [4, 512, 2048], replicated
- w_out: float32 [4, 2048, 512], replicated
Outputs:
- output 1: float32 [4, 512, 2048], replicated
- output 2: float32 [4, 2048, 512], replicated
- output 3: float32 [], replicated
All inputs are finite; a program needn't handle non-finite values.
Results may differ from the reference program's by a relative error of at most 0.00108718.
Values are sent between devices in bfloat16 or wider.
A program may use at most 1 GiB of HBM per device.

```python
import jax
import jax.numpy as jnp
import math
from jax import lax

D = 512
FF = 2048
SEQ = 196
LAYERS = 4
IMGS_DEV = 8
DEVICES = 32
IMAGES = IMGS_DEV * DEVICES
TOKENS = IMAGES * SEQ
BLOCK_ROWS = IMGS_DEV * SEQ
INV_COUNT = 1.0 / (TOKENS * D)
RHO_REL = 0.1
RADIUS = RHO_REL * math.sqrt(LAYERS * FF + D)
LEARN_RATE = 8.0
SQRT_HALF = 0.7071067811865476
INV_SQRT_2PI = 0.3989422804014327


def setup_inputs(seed: int = 0) -> dict:
    root_key = jax.random.key(seed)
    subkeys = jax.random.split(root_key, 8)
    img_shift = 0.8 * jax.random.normal(subkeys[0], (IMAGES, 1, D), jnp.float32)
    img_gain = jnp.exp(0.3 * jax.random.normal(subkeys[1], (IMAGES, 1, 1), jnp.float32))
    images = jax.random.normal(subkeys[2], (IMAGES, SEQ, D), jnp.float32) * img_gain + img_shift
    tgt_shift = 0.5 * jax.random.normal(subkeys[3], (1, 1, D), jnp.float32) + 0.8 * jax.random.normal(subkeys[4], (IMAGES, 1, D), jnp.float32)
    targets = jax.random.normal(subkeys[5], (IMAGES, SEQ, D), jnp.float32) + tgt_shift
    w_in = jax.random.normal(subkeys[6], (LAYERS, D, FF), jnp.float32) * D ** -0.5
    w_out = jax.random.normal(subkeys[7], (LAYERS, FF, D), jnp.float32) * (FF * LAYERS) ** -0.5
    return {'images': images.astype(jnp.bfloat16), 'targets': targets.astype(jnp.bfloat16), 'w_in': w_in, 'w_out': w_out}


def gelu_fn(pre_act):
    return 0.5 * pre_act * (1.0 + lax.erf(pre_act * SQRT_HALF))


def gelu_slope(pre_act):
    cdf_part = 0.5 * (1.0 + lax.erf(pre_act * SQRT_HALF))
    return cdf_part + pre_act * INV_SQRT_2PI * jnp.exp(-0.5 * pre_act * pre_act)


def layer_forward(hidden, weights):
    w_in_l, w_out_l = weights
    pre_act = jnp.dot(hidden, w_in_l, preferred_element_type=jnp.float32).astype(jnp.bfloat16)
    post_act = gelu_fn(pre_act.astype(jnp.float32)).astype(jnp.bfloat16)
    mlp_out = jnp.dot(post_act, w_out_l, preferred_element_type=jnp.float32)
    new_hidden = (hidden.astype(jnp.float32) + mlp_out).astype(jnp.bfloat16)
    return new_hidden, (hidden, pre_act, post_act)


def layer_backward(d_hidden, inputs_l):
    hidden, pre_act, post_act, w_in_l, w_out_l = inputs_l
    grad_out = jnp.dot(post_act.T, d_hidden, preferred_element_type=jnp.float32)
    d_act = jnp.dot(d_hidden, w_out_l.T, preferred_element_type=jnp.float32)
    d_pre = (d_act * gelu_slope(pre_act.astype(jnp.float32))).astype(jnp.bfloat16)
    grad_in = jnp.dot(hidden.T, d_pre, preferred_element_type=jnp.float32)
    d_prev = (d_hidden.astype(jnp.float32) + jnp.dot(d_pre, w_in_l.T, preferred_element_type=jnp.float32)).astype(jnp.bfloat16)
    return d_prev, (grad_in, grad_out)


def block_grads(x_rows, y_rows, w_in_bf, w_out_bf):
    top_hidden, saved_acts = lax.scan(layer_forward, x_rows, (w_in_bf, w_out_bf))
    resid_err = top_hidden.astype(jnp.float32) - y_rows.astype(jnp.float32)
    d_top = (resid_err * INV_COUNT).astype(jnp.bfloat16)
    hiddens, pre_acts, post_acts = saved_acts
    _, grads = lax.scan(layer_backward, d_top, (hiddens, pre_acts, post_acts, w_in_bf, w_out_bf), reverse=True)
    return 0.5 * jnp.sum(resid_err * resid_err), grads[0], grads[1]


def full_grads(images, targets, w_in_bf, w_out_bf):
    x_blocks = images.reshape(DEVICES, BLOCK_ROWS, D)
    y_blocks = targets.reshape(DEVICES, BLOCK_ROWS, D)

    def accumulate(totals, block_pair):
        loss_blk, gin_blk, gout_blk = block_grads(block_pair[0], block_pair[1], w_in_bf, w_out_bf)
        return (totals[0] + loss_blk, totals[1] + gin_blk, totals[2] + gout_blk), None

    init_carry = (jnp.zeros((), jnp.float32), jnp.zeros((LAYERS, D, FF), jnp.float32), jnp.zeros((LAYERS, FF, D), jnp.float32))
    totals, _ = lax.scan(accumulate, init_carry, (x_blocks, y_blocks))
    return totals


def reference(images, targets, w_in, w_out):
    _, grad_in, grad_out = full_grads(images, targets, w_in.astype(jnp.bfloat16), w_out.astype(jnp.bfloat16))
    grad_norm = jnp.sqrt(jnp.sum(grad_in * grad_in) + jnp.sum(grad_out * grad_out))
    step_scale = RADIUS / grad_norm
    pert_in = (w_in + step_scale * grad_in).astype(jnp.bfloat16)
    pert_out = (w_out + step_scale * grad_out).astype(jnp.bfloat16)
    loss_sum, grad2_in, grad2_out = full_grads(images, targets, pert_in, pert_out)
    return (w_in - LEARN_RATE * grad2_in, w_out - LEARN_RATE * grad2_out, loss_sum * INV_COUNT)
```

```python
import math

import jax
import jax.numpy as jnp
from jax import lax
from jax.experimental import pallas as pl
from jax.experimental.pallas import tpu as pltpu
from jax.sharding import PartitionSpec as P

MESH = pl.DeviceIdType.MESH
f32 = jnp.float32
bf16 = jnp.bfloat16
RHO_REL = 0.1
LEARN_RATE = 8.0
SQRT_HALF = 0.7071067811865476
INV_SQRT_PI = 0.5641895835477563
LOG2_E = 1.4426950408889634
LAYERS, D, F = 4, 512, 2048
HALF = F // 2
W = 256
NU = 32
ROWS = (512, 256, 128, 64, 32)
VMEM_LIMIT = 62 * 2**20

ANY = pl.BlockSpec(memory_space=pl.ANY)
DMA = pltpu.SemaphoreType.DMA


def aligned(value, multiple):
    return pl.multiple_of(value, multiple)


def gelu(x):
    return (0.5 * x) * (1.0 + lax.erf(x * SQRT_HALF))


def gelu_slope(x):
    z = x * SQRT_HALF
    return (0.5 + 0.5 * lax.erf(z)) + (z * INV_SQRT_PI) * jnp.exp2(z * z * (-LOG2_E))


def coords():
    z, y, dd = lax.axis_index("model"), lax.axis_index("sub"), lax.axis_index("data")
    return z, y, dd // 2, dd % 2


class Cube:
    def __init__(self):
        z, y, x, c = coords()
        fx, fy = 1 - 2 * x, 1 - 2 * y
        self.core = c
        self.devs = (
            (z, y, x * 2 + (1 - c)),
            (z, y + c * fy, (x + (1 - c) * fx) * 2 + c),
            (z + 1 - 2 * (z % 2), y, x * 2 + c),
            (z, y + (1 - c) * fy, (x + c * fx) * 2 + c),
            ((z + 2) % 4, y, x * 2 + c),
        )
        bits = (x * (1 - c) + y * c, z % 2, y * (1 - c) + x * c, z // 2)
        self.keep, self.give, base = [], [], 0
        for i in range(4):
            half = ROWS[i + 1]
            self.keep.append(base + bits[i] * half)
            self.give.append(base + (1 - bits[i]) * half)
            base = base + bits[i] * half

    def barrier(self):
        sem = pltpu.get_barrier_semaphore()
        for dev in self.devs:
            pl.semaphore_signal(sem, inc=1, device_id=dev, device_id_type=MESH)
        pl.semaphore_wait(sem, len(self.devs))


def remote(src, dst, send_sem, recv_sem, dev):
    return pltpu.make_async_remote_copy(
        src_ref=src, dst_ref=dst, send_sem=send_sem, recv_sem=recv_sem, device_id=dev, device_id_type=MESH
    )


class ReduceScatter:
    NSD, ND, NA, N, LAG = 4, 8, 16, 8, 2
    TICKS = NU + 4 * LAG

    @classmethod
    def scratch(cls):
        n = cls.N
        return [
            pltpu.VMEM((cls.NSD, 512, W), f32),
            pltpu.VMEM((cls.NA, 512, W), f32),
            pltpu.VMEM((cls.ND, 512, W), f32),
            pltpu.VMEM((n, 256, W), f32),
            pltpu.VMEM((n, 128, W), f32),
            pltpu.VMEM((n, 64, W), f32),
            pltpu.VMEM((n, 32, W), f32),
            DMA((cls.NSD,)),
            DMA((cls.ND,)),
            DMA((4, n)),
            DMA((4, n)),
            pltpu.SemaphoreType.REGULAR,
        ]

    def __init__(self, cube, refs):
        self.cube = cube
        (self.out, self.acc, self.inc, r1, r2, r3, r4, self.dsend, self.drecv, self.ssem, self.rsem, self.credit) = refs
        self.recv = (r1, r2, r3, r4)

    def core_copy(self, k):
        return remote(
            self.out.at[k % self.NSD],
            self.inc.at[k % self.ND],
            self.dsend.at[k % self.NSD],
            self.drecv.at[k % self.ND],
            self.cube.devs[0],
        )

    def copy(self, i, k):
        n = ROWS[i + 1]
        return remote(
            self.acc.at[k % self.NA, pl.ds(aligned(self.cube.give[i], n), n), :],
            self.recv[i].at[k % self.N],
            self.ssem.at[i, k % self.N],
            self.rsem.at[i, k % self.N],
            self.cube.devs[i + 1],
        )

    def before_write(self, k):
        @pl.when(k >= self.NSD)
        def _():
            self.core_copy(k - self.NSD).wait_send()

    def push(self, k):
        @pl.when(k >= self.ND)
        def _():
            pl.semaphore_wait(self.credit, 1)

        self.core_copy(k).start()

    def finish(self):
        for k in range(NU - self.NSD, NU):
            self.core_copy(k).wait_send()
        pl.semaphore_wait(self.credit, self.ND)

    def tick(self, t, final):
        @pl.when((t >= 0) & (t < NU))
        def _():
            self.core_copy(t).wait_recv()
            self.acc[t % self.NA] = self.acc[t % self.NA] + self.inc[t % self.ND]
            pl.semaphore_signal(self.credit, inc=1, device_id=self.cube.devs[0], device_id_type=MESH)
            self.copy(0, t).start()

        for i in range(4):
            u = t - (i + 1) * self.LAG

            @pl.when((u >= 0) & (u < NU))
            def _(i=i, u=u):
                n = ROWS[i + 1]
                self.copy(i, u).wait()
                rows = pl.ds(aligned(self.cube.keep[i], n), n)
                value = self.acc[u % self.NA, rows, :] + self.recv[i][u % self.N]
                if i < 3:
                    self.acc[u % self.NA, rows, :] = value
                    self.copy(i + 1, u).start()
                else:
                    final(u, value)


class Gather:
    N = 8

    def __init__(self, cube, units, lag, block, ssem, rsem, first=None, local=None):
        self.cube, self.units, self.lag, self.block = cube, units, lag, block
        self.ssem, self.rsem, self.first, self.local = ssem, rsem, first, local

    @classmethod
    def scratch(cls):
        return [DMA((5, cls.N)), DMA((5, cls.N))]

    def copy(self, a, u):
        n = ROWS[4 - a]
        base = 0 if a == 4 else aligned(self.cube.keep[3 - a], n)
        here = self.block(u, pl.ds(base, n))
        src = self.first(u) if a == 0 and self.first is not None else here
        return remote(src, here, self.ssem.at[a, u % self.N], self.rsem.at[a, u % self.N], self.cube.devs[4 - a])

    def tick(self, t):
        for a in range(6):
            u = t - a * self.lag

            @pl.when((u >= 0) & (u < self.units))
            def _(a=a, u=u):
                if a > 0:
                    self.copy(a - 1, u).wait()
                if self.local is not None:
                    if a == 0:
                        self.local(u).start()
                    elif a == 1:
                        self.local(u).wait()
                if a < 5:
                    self.copy(a, u).start()


def small_scratch():
    return [pltpu.VMEM((6, 8, 128), f32), pltpu.VMEM((5, 8, 128), f32), DMA((5,)), DMA((5,))]


def small_step(cube, refs, i):
    mine, theirs, ssem, rsem = refs

    def copy(j):
        return remote(mine.at[j], theirs.at[j], ssem.at[j], rsem.at[j], cube.devs[j])

    if i > 0:
        copy(i - 1).wait()
        mine[i] = mine[i - 1] + theirs[i - 1]
    if i < 5:
        copy(i).start()


def fold(rows):
    out = jnp.zeros((8, 128), f32)
    for r in range(0, rows.shape[0], 8):
        for q in range(0, rows.shape[1], 128):
            out = out + rows[r : r + 8, q : q + 128]
    return out


def dot(a, b, ca=1, cb=0):
    return lax.dot_general(a, b, (((ca,), (cb,)), ((), ())), preferred_element_type=f32)


def forward_in(half, h_ref, cur, wa, u_ref, a_ref, rows):
    acc = dot(h_ref[cur, pl.ds(aligned(half * rows, 16), rows), :], wa)
    u = acc.astype(bf16)
    u_ref[half] = u
    a_ref[half] = gelu(u.astype(f32)).astype(bf16)


def forward_out(half, h_ref, cur, wb, transposed, a_ref, rows):
    rs = pl.ds(aligned(half * rows, 16), rows)
    acc = dot(a_ref[half], wb, 1, 1 if transposed else 0)
    h_ref[1 - cur, rs, :] = (h_ref[cur, rs, :].astype(f32) + acc).astype(bf16)


def forward_kernel(
    tokens, x_in, y_in, win, wout, hs, us, acts, d_out, a_out, b_out, shard_out,
    h, u, a, y, st_a, st_b, wa, wb, shard, turn, sx, sy, sa, sb, su, sact, sh, sao, sbo, sd, ss,
):
    rows = tokens // 2
    cube = Cube()
    row = cube.keep[3]
    col = cube.core * HALF

    def load_a(l):
        return pltpu.make_async_copy(win.at[l], st_a, sa)

    def load_b(l):
        return pltpu.make_async_copy(wout.at[l], st_b, sb)

    def save_u(l, r):
        return pltpu.make_async_copy(u.at[r], us.at[l, pl.ds(aligned(r * rows, 16), rows), :], su.at[r])

    def save_act(l, r):
        return pltpu.make_async_copy(a.at[r], acts.at[l, pl.ds(aligned(r * rows, 16), rows), :], sact.at[r])

    def save_h(l):
        return pltpu.make_async_copy(h.at[l % 2], hs.at[l], sh.at[l % 2])

    def save_a(l):
        return pltpu.make_async_copy(wa.at[l % 2], a_out.at[l], sao.at[l % 2])

    def save_b(l):
        return pltpu.make_async_copy(wb.at[l % 2], b_out.at[l], sbo.at[l % 2])

    copy_x = pltpu.make_async_copy(x_in, h.at[0], sx)
    copy_y = pltpu.make_async_copy(y_in, y, sy)
    load_a(0).start()
    copy_x.start()
    load_b(0).start()
    copy_y.start()
    copy_x.wait()
    save_h(0).start()

    def layer(l, carry):
        cur = l % 2
        k0 = (LAYERS - 1 - l) * 8

        @pl.when(l >= 2)
        def _():
            save_a(l - 2).wait()
            save_b(l - 2).wait()

        load_a(l).wait()

        def convert_a(i, carry):
            rs = pl.ds(aligned(i * 64, 64), 64)
            wa[cur, rs, :] = st_a[rs, :].astype(bf16)
            return carry

        lax.fori_loop(0, D // 64, convert_a, 0)
        for j in range(4):
            shard[k0 + 4 + j] = st_a[pl.ds(aligned(row, 32), 32), pl.ds(aligned(col + j * W, W), W)]
        save_a(l).start()

        @pl.when(l < LAYERS - 1)
        def _():
            load_a(l + 1).start()

        load_b(l).wait()

        def convert_b(i, carry):
            rs = pl.ds(aligned(i * 256, 256), 256)
            wb[cur, rs, :] = st_b[rs, :].astype(bf16)
            return carry

        lax.fori_loop(0, F // 256, convert_b, 0)
        for j in range(4):
            lanes = pl.ds(aligned((row // 128) * 128, 128), 128)
            turn[...] = st_b[pl.ds(aligned(col + j * W, W), W), lanes].T
            shard[k0 + j] = turn[pl.ds(aligned(row % 128, 32), 32), :]
        save_b(l).start()

        @pl.when(l < LAYERS - 1)
        def _():
            load_b(l + 1).start()

        def half_in(r, carry):
            @pl.when(l >= 1)
            def _():
                save_u(l - 1, r).wait()
                save_act(l - 1, r).wait()

            forward_in(r, h, cur, wa[cur], u, a, rows)
            save_u(l, r).start()
            save_act(l, r).start()
            return carry

        lax.fori_loop(0, 2, half_in, 0)

        @pl.when(l >= 1)
        def _():
            save_h(l - 1).wait()

        def half_out(r, carry):
            forward_out(r, h, cur, wb[cur], False, a, rows)
            return carry

        lax.fori_loop(0, 2, half_out, 0)

        @pl.when(l < LAYERS - 1)
        def _():
            save_h(l + 1).start()

        return carry

    lax.fori_loop(0, LAYERS, layer, 0)
    copy_y.wait()
    inv_count = 1.0 / (tokens * 32 * D)
    for r in range(2):
        rs = slice(r * rows, (r + 1) * rows)
        y[rs, :] = ((h[0, rs, :].astype(f32) - y[rs, :].astype(f32)) * inv_count).astype(bf16)
    save_d = pltpu.make_async_copy(y, d_out, sd)
    save_s = pltpu.make_async_copy(shard, shard_out, ss)
    save_d.start()
    save_s.start()
    for r in range(2):
        save_u(LAYERS - 1, r).wait()
        save_act(LAYERS - 1, r).wait()
        save_a(LAYERS - 2 + r).wait()
        save_b(LAYERS - 2 + r).wait()
    save_h(LAYERS - 1).wait()
    save_d.wait()
    save_s.wait()


def gather_forward_kernel(
    tokens, x_in, y_in, g_in, shard_in, norm_in, hs, us, acts, d_out, w_out, loss_out,
    h, u, a, y, wts, g, shard, norm, loss, sx, sy, sl, su, sact, sh, sw, sd, sloss, gsend, grecv,
):
    rows = tokens // 2
    radius = RHO_REL * math.sqrt(LAYERS * F + D)
    cube = Cube()
    row = cube.keep[3]
    col = cube.core * HALF
    lag = 1

    def save_u(l, r):
        return pltpu.make_async_copy(u.at[r], us.at[l, pl.ds(aligned(r * rows, 16), rows), :], su.at[r])

    def save_act(l, r):
        return pltpu.make_async_copy(a.at[r], acts.at[l, pl.ds(aligned(r * rows, 16), rows), :], sact.at[r])

    def save_h(l):
        return pltpu.make_async_copy(h.at[l % 2], hs.at[l], sh.at[l % 2])

    def save_w(m):
        return pltpu.make_async_copy(wts.at[m], w_out.at[m], sw.at[m])

    loads = [pltpu.make_async_copy(s, d, sl.at[i]) for i, (s, d) in enumerate(((norm_in, norm), (g_in, g), (shard_in, shard)))]
    copy_x = pltpu.make_async_copy(x_in, h.at[0], sx)
    copy_y = pltpu.make_async_copy(y_in, y, sy)
    for load in loads:
        load.start()
    copy_x.start()
    copy_y.start()
    cube.barrier()
    for load in loads:
        load.wait()
    total = jnp.sum(jnp.sum(norm[...], axis=0, keepdims=True), axis=1, keepdims=True)
    scale = radius / jnp.sqrt(total)

    def perturb(m, carry):
        k0 = (LAYERS - 1 - m // 2) * 8 + 4 - (m % 2) * 4
        for j in range(4):
            value = shard[k0 + j] + scale * g[k0 + j]
            wts[m, pl.ds(aligned(row, 32), 32), pl.ds(aligned(col + j * W, W), W)] = value.astype(bf16)
        return carry

    lax.fori_loop(0, 2 * LAYERS, perturb, 0)

    def block(unit, rs):
        return wts.at[unit // 2, rs, pl.ds(aligned(col + (unit % 2) * 512, 512), 512)]

    gather = Gather(cube, 4 * LAYERS, lag, block, gsend, grecv)
    lead = 5 * lag + 2

    def first(t, carry):
        gather.tick(t)
        return carry

    lax.fori_loop(0, lead, first, 0)
    copy_x.wait()
    save_h(0).start()

    def layer(l, carry):
        cur = l % 2
        save_w(2 * l).start()

        def half_in(r, carry):
            @pl.when(l >= 1)
            def _():
                save_u(l - 1, r).wait()
                save_act(l - 1, r).wait()

            forward_in(r, h, cur, wts[2 * l], u, a, rows)
            save_u(l, r).start()
            save_act(l, r).start()
            gather.tick(lead + 4 * l + r)
            return carry

        lax.fori_loop(0, 2, half_in, 0)
        save_w(2 * l + 1).start()

        @pl.when(l >= 1)
        def _():
            save_h(l - 1).wait()

        def half_out(r, carry):
            forward_out(r, h, cur, wts[2 * l + 1], True, a, rows)
            gather.tick(lead + 4 * l + 2 + r)
            return carry

        lax.fori_loop(0, 2, half_out, 0)

        @pl.when(l < LAYERS - 1)
        def _():
            save_h(l + 1).start()

        return carry

    lax.fori_loop(0, LAYERS, layer, 0)
    copy_y.wait()
    inv_count = 1.0 / (tokens * 32 * D)
    part = jnp.zeros((1, D), f32)
    for r in range(2):
        rs = slice(r * rows, (r + 1) * rows)
        diff = h[0, rs, :].astype(f32) - y[rs, :].astype(f32)
        y[rs, :] = (diff * inv_count).astype(bf16)
        part = part + jnp.sum(diff * diff, axis=0, keepdims=True)
    lanes = part[:, :128] + part[:, 128:256] + part[:, 256:384] + part[:, 384:]
    top = lax.broadcasted_iota(jnp.int32, (8, 128), 0) == 0
    loss[...] = jnp.where(top, jnp.broadcast_to(lanes, (8, 128)), 0.0)
    save_d = pltpu.make_async_copy(y, d_out, sd)
    save_loss = pltpu.make_async_copy(loss, loss_out, sloss)
    save_d.start()
    save_loss.start()
    for r in range(2):
        save_u(LAYERS - 1, r).wait()
        save_act(LAYERS - 1, r).wait()
    for m in range(2 * LAYERS):
        save_w(m).wait()
    save_h(LAYERS - 1).wait()
    save_d.wait()
    save_loss.wait()


def backward_compute(tokens, refs, cube, scatter, tick, load_a, load_b, transposed):
    (hs, us, acts, d_in, h, u, a, d, wa, wb, sh, su, sact, sd, sa, sb) = refs
    rows = tokens // 2
    own, other = cube.core * HALF, (1 - cube.core) * HALF

    def load(src, dst, sem):
        return pltpu.make_async_copy(src, dst, sem)

    def load_h(l):
        return load(hs.at[l], h, sh)

    def load_u(l):
        return load(us.at[l], u, su)

    def load_act(l):
        return load(acts.at[l], a, sact)

    load(d_in, d, sd).start()
    load_act(LAYERS - 1).start()
    load_u(LAYERS - 1).start()
    load_b(LAYERS - 1).start()
    load_h(LAYERS - 1).start()
    load_a(LAYERS - 1).start()
    cube.barrier()
    load(d_in, d, sd).wait()

    def produce(k, lhs, src, pair):
        scatter.before_write(k)
        scatter.before_write(k + 1)
        value = dot(lhs[...], src[:, pl.ds(aligned(other + pair * 512, 512), 512)], 0, 0)
        scatter.out[k % scatter.NSD] = value[:, :W]
        scatter.out[(k + 1) % scatter.NSD] = value[:, W:]
        scatter.push(k)
        scatter.push(k + 1)
        value = dot(lhs[...], src[:, pl.ds(aligned(own + pair * 512, 512), 512)], 0, 0)
        scatter.acc[k % scatter.NA] = value[:, :W]
        scatter.acc[(k + 1) % scatter.NA] = value[:, W:]

    def layer(i, carry):
        l = LAYERS - 1 - i
        more = i < LAYERS - 1
        load_act(l).wait()

        def out_pair(p, carry):
            produce(i * 8 + 2 * p, d, a, p)
            tick(i * 8 + p)
            return carry

        lax.fori_loop(0, 2, out_pair, 0)

        @pl.when(more)
        def _():
            load_act(l - 1).start()

        load_u(l).wait()
        load_b(l).wait()

        def slope_half(r, carry):
            rs = pl.ds(aligned(r * rows, 16), rows)
            for n in range(2):
                cs = slice(n * HALF, (n + 1) * HALF)
                if transposed:
                    da = dot(d[rs, :], wb[:, cs])
                else:
                    da = dot(d[rs, :], wb[cs, :], 1, 1)
                u[rs, cs] = (da * gelu_slope(u[rs, cs].astype(f32))).astype(bf16)
            tick(i * 8 + 2 + r)
            return carry

        lax.fori_loop(0, 2, slope_half, 0)

        @pl.when(more)
        def _():
            load_b(l - 1).start()

        load_h(l).wait()

        def in_pair(p, carry):
            produce(i * 8 + 4 + 2 * p, h, u, p)
            tick(i * 8 + 4 + p)
            return carry

        lax.fori_loop(0, 2, in_pair, 0)
        load_a(l).wait()

        @pl.when(more)
        def _():
            load_h(l - 1).start()

        def back_half(r, carry):
            @pl.when(more)
            def _():
                rs = pl.ds(aligned(r * rows, 16), rows)
                acc = dot(u[rs, :], wa[...], 1, 1)
                d[rs, :] = (d[rs, :].astype(f32) + acc).astype(bf16)

            tick(i * 8 + 6 + r)
            return carry

        lax.fori_loop(0, 2, back_half, 0)

        @pl.when(more)
        def _():
            load_a(l - 1).start()
            load_u(l - 1).start()

        return carry

    lax.fori_loop(0, LAYERS, layer, 0)


LEAD = 1


def backward_scatter_kernel(
    tokens, hs, us, acts, d_in, a_in, b_in, g_out, norm_out,
    h, u, a, d, wa, wb, sh, su, sact, sd, sa, sb, g, norm, sg, *refs,
):
    cube = Cube()
    scatter = ReduceScatter(cube, refs[:12])
    small = refs[12:]
    norm[...] = jnp.zeros_like(norm)

    def final(unit, value):
        g[unit] = value
        norm[...] += value * value

    def tick(t):
        scatter.tick(t - LEAD, final)

    backward_compute(
        tokens, (hs, us, acts, d_in, h, u, a, d, wa, wb, sh, su, sact, sd, sa, sb), cube, scatter, tick,
        lambda l: pltpu.make_async_copy(a_in.at[l], wa, sa), lambda l: pltpu.make_async_copy(b_in.at[l], wb, sb), False,
    )

    def rest(t, carry):
        tick(t)
        return carry

    lax.fori_loop(NU, scatter.TICKS + LEAD, rest, 0)
    save_g = pltpu.make_async_copy(g, g_out, sg.at[0])
    save_g.start()
    small[0][0] = fold(norm[...])
    for i in range(6):
        small_step(cube, small, i)
    save_n = pltpu.make_async_copy(small[0].at[5], norm_out, sg.at[1])
    save_n.start()
    scatter.finish()
    save_g.wait()
    save_n.wait()


def backward_update_kernel(
    tokens, hs, us, acts, d_in, w_in, shard_in, loss_in, new_out, loss_out,
    h, u, a, d, wa, wb, sh, su, sact, sd, sa, sb, shard, sg, slocal, gsend, grecv, *refs,
):
    cube = Cube()
    scatter = ReduceScatter(cube, refs[:12])
    small = refs[12:]
    row = cube.keep[3]
    lag = 2
    late = 4 * scatter.LAG + 1
    load_s = pltpu.make_async_copy(shard_in, shard, sg.at[0])
    load_l = pltpu.make_async_copy(loss_in, small[0].at[0], sg.at[1])
    load_s.start()
    load_l.start()

    def block(unit, rs):
        return new_out.at[unit, cube.core, rs, :]

    def local(unit):
        return pltpu.make_async_copy(
            shard.at[unit], block(unit, pl.ds(aligned(row, 32), 32)), slocal.at[unit % Gather.N]
        )

    gather = Gather(cube, NU, lag, block, gsend, grecv, lambda unit: shard.at[unit], local)

    def final(unit, value):
        shard[unit] = shard[unit] - LEARN_RATE * value

    def tick(t):
        for i in range(6):
            @pl.when(t == i)
            def _(i=i):
                if i == 0:
                    load_s.wait()
                    load_l.wait()
                small_step(cube, small, i)

        scatter.tick(t - LEAD, final)
        gather.tick(t - LEAD - late)

    backward_compute(
        tokens, (hs, us, acts, d_in, h, u, a, d, wa, wb, sh, su, sact, sd, sa, sb), cube, scatter, tick,
        lambda l: pltpu.make_async_copy(w_in.at[2 * l], wa, sa),
        lambda l: pltpu.make_async_copy(w_in.at[2 * l + 1], wb, sb), True,
    )

    def rest(t, carry):
        tick(t)
        return carry

    lax.fori_loop(NU, NU + late + LEAD + 5 * lag, rest, 0)
    save_l = pltpu.make_async_copy(small[0].at[5], loss_out, sg.at[1])
    save_l.start()
    scatter.finish()
    save_l.wait()


def place_kernel(out_part, in_part, new_in, new_out):
    new_in[...] = in_part[0, 0][None]
    new_out[...] = out_part[0, 0].T[None]


def solution(mesh):
    axes = tuple(mesh.axis_names)
    spec = P(axes, None, None)
    S = jax.ShapeDtypeStruct

    def step(images, targets, w_in, w_out):
        tokens = images.shape[0] * images.shape[1]
        rows = tokens // 2
        x = images.reshape(tokens, D)
        y = targets.reshape(tokens, D)
        saved = [S((LAYERS, tokens, D), bf16), S((LAYERS, tokens, F), bf16), S((LAYERS, tokens, F), bf16), S((tokens, D), bf16)]
        VM = pltpu.VMEM
        fwd_bufs = [VM((2, tokens, D), bf16), VM((2, rows, F), bf16), VM((2, rows, F), bf16), VM((tokens, D), bf16)]
        bwd_bufs = [VM((tokens, D), bf16), VM((tokens, F), bf16), VM((tokens, F), bf16), VM((tokens, D), bf16)]

        def call(kernel, outs, scratch, *args, collective=None):
            params = dict(vmem_limit_bytes=VMEM_LIMIT)
            if collective is not None:
                params.update(collective_id=collective, has_side_effects=True)
            return pl.pallas_call(
                lambda *refs: kernel(tokens, *refs),
                out_shape=outs,
                in_specs=[ANY] * len(args),
                out_specs=[ANY] * len(outs),
                scratch_shapes=scratch,
                compiler_params=pltpu.CompilerParams(**params),
                name=kernel.__name__,
            )(*args)

        hs, us, acts, d_top, a_bf, b_bf, shard = call(
            forward_kernel,
            saved + [S((LAYERS, D, F), bf16), S((LAYERS, F, D), bf16), S((NU, 32, W), f32)],
            fwd_bufs
            + [VM((D, F), f32), VM((F, D), f32), VM((2, D, F), bf16), VM((2, F, D), bf16), VM((NU, 32, W), f32), VM((128, W), f32)]
            + [DMA, DMA, DMA, DMA, DMA((2,)), DMA((2,)), DMA((2,)), DMA((2,)), DMA((2,)), DMA, DMA],
            x, y, w_in, w_out,
        )
        grads, norm = call(
            backward_scatter_kernel,
            [S((NU, 32, W), f32), S((8, 128), f32)],
            bwd_bufs
            + [VM((D, F), bf16), VM((F, D), bf16)]
            + [DMA] * 6
            + [VM((NU, 32, W), f32), VM((32, W), f32), DMA((2,))]
            + ReduceScatter.scratch()
            + small_scratch(),
            hs, us, acts, d_top, a_bf, b_bf,
            collective=1,
        )
        hs, us, acts, d_top, wts, loss = call(
            gather_forward_kernel,
            saved + [S((2 * LAYERS, D, F), bf16), S((8, 128), f32)],
            fwd_bufs
            + [VM((2 * LAYERS, D, F), bf16), VM((NU, 32, W), f32), VM((NU, 32, W), f32), VM((8, 128), f32), VM((8, 128), f32)]
            + [DMA, DMA, DMA((3,)), DMA((2,)), DMA((2,)), DMA((2,)), DMA((2 * LAYERS,)), DMA, DMA]
            + Gather.scratch(),
            x, y, grads, shard, norm,
            collective=2,
        )
        parts, loss = call(
            backward_update_kernel,
            [S((NU, 2, D, W), f32), S((8, 128), f32)],
            bwd_bufs
            + [VM((D, F), bf16), VM((D, F), bf16)]
            + [DMA] * 6
            + [VM((NU, 32, W), f32), DMA((2,)), DMA((Gather.N,))]
            + Gather.scratch()
            + ReduceScatter.scratch()
            + small_scratch(),
            hs, us, acts, d_top, wts, shard, loss,
            collective=3,
        )

        def part_spec(offset):
            return pl.BlockSpec((1, 1, D, W), lambda i: ((LAYERS - 1 - i // 8) * 8 + offset + i % 4, (i // 4) % 2, 0, 0))

        new_in, new_out = pl.pallas_call(
            place_kernel,
            out_shape=[S((LAYERS, D, F), f32), S((LAYERS, F, D), f32)],
            grid=(NU,),
            in_specs=[part_spec(0), part_spec(4)],
            out_specs=[pl.BlockSpec((1, D, W), lambda i: (i // 8, 0, i % 8)), pl.BlockSpec((1, W, D), lambda i: (i // 8, i % 8, 0))],
            name="place",
        )(parts, parts)
        inv_count = 1.0 / (tokens * math.prod(mesh.shape.values()) * D)
        return new_in, new_out, (0.5 * jnp.sum(loss)) * inv_count

    return jax.shard_map(step, mesh=mesh, in_specs=(spec, spec, P(), P()), out_specs=(P(), P(), P()), check_vma=False)
```

```python
import math

import jax
import jax.numpy as jnp
from jax import lax
from jax.experimental import pallas as pl
from jax.experimental.pallas import tpu as pltpu
from jax.sharding import PartitionSpec as P

MESH = pl.DeviceIdType.MESH
f32 = jnp.float32
bf16 = jnp.bfloat16
RHO_REL = 0.1
LEARN_RATE = 8.0
SQRT_HALF = 0.7071067811865476
INV_SQRT_PI = 0.5641895835477563
LOG2_E = 1.4426950408889634
LAYERS, D, F = 4, 512, 2048
DEVICES = 32
HALF = F // 2
W = 256
NU = 32
ROWS = (512, 256, 128, 64, 32)
VMEM_LIMIT = 62 * 2**20

ANY = pl.BlockSpec(memory_space=pl.ANY)
DMA = pltpu.SemaphoreType.DMA


def aligned(value, multiple):
    return pl.multiple_of(value, multiple)


def gelu(x):
    return (0.5 * x) * (1.0 + lax.erf(x * SQRT_HALF))


def gelu_slope(x):
    z = x * SQRT_HALF
    return (0.5 + 0.5 * lax.erf(z)) + (z * INV_SQRT_PI) * jnp.exp2(z * z * (-LOG2_E))


def coords():
    z, y, dd = lax.axis_index("model"), lax.axis_index("sub"), lax.axis_index("data")
    return z, y, dd // 2, dd % 2


class Cube:
    def __init__(self):
        z, y, x, c = coords()
        fx, fy = 1 - 2 * x, 1 - 2 * y
        self.core = c
        self.devs = (
            (z, y, x * 2 + (1 - c)),
            (z, y + c * fy, (x + (1 - c) * fx) * 2 + c),
            (z + 1 - 2 * (z % 2), y, x * 2 + c),
            (z, y + (1 - c) * fy, (x + c * fx) * 2 + c),
            ((z + 2) % 4, y, x * 2 + c),
        )
        bits = (x * (1 - c) + y * c, z % 2, y * (1 - c) + x * c, z // 2)
        self.keep, self.give, base = [], [], 0
        for i in range(4):
            half = ROWS[i + 1]
            self.keep.append(base + bits[i] * half)
            self.give.append(base + (1 - bits[i]) * half)
            base = base + bits[i] * half

        self.me = (z * 2 + y) * 4 + x * 2 + c

    def other(self, i):
        n = lax.rem(self.me + i, DEVICES)
        return (n // 8, (n // 4) % 2, n % 4), n


def remote(src, dst, send_sem, recv_sem, dev):
    return pltpu.make_async_remote_copy(
        src_ref=src, dst_ref=dst, send_sem=send_sem, recv_sem=recv_sem, device_id=dev, device_id_type=MESH
    )


class ReduceScatter:
    NSD, ND, NA, N, LAG = 4, 8, 16, 8, 2
    TICKS = NU + 4 * LAG

    @classmethod
    def scratch(cls):
        n = cls.N
        return [
            pltpu.VMEM((cls.NSD, 512, W), f32),
            pltpu.VMEM((cls.NA, 512, W), f32),
            pltpu.VMEM((cls.ND, 512, W), f32),
            pltpu.VMEM((n, 256, W), f32),
            pltpu.VMEM((n, 128, W), f32),
            pltpu.VMEM((n, 64, W), f32),
            pltpu.VMEM((n, 32, W), f32),
            DMA((cls.NSD,)),
            DMA((cls.ND,)),
            DMA((4, n)),
            DMA((4, n)),
            pltpu.SemaphoreType.REGULAR,
        ]

    def __init__(self, cube, refs):
        self.cube = cube
        (self.out, self.acc, self.inc, r1, r2, r3, r4, self.dsend, self.drecv, self.ssem, self.rsem, self.credit) = refs
        self.recv = (r1, r2, r3, r4)

    def core_copy(self, k):
        return remote(
            self.out.at[k % self.NSD],
            self.inc.at[k % self.ND],
            self.dsend.at[k % self.NSD],
            self.drecv.at[k % self.ND],
            self.cube.devs[0],
        )

    def copy(self, i, k):
        n = ROWS[i + 1]
        return remote(
            self.acc.at[k % self.NA, pl.ds(aligned(self.cube.give[i], n), n), :],
            self.recv[i].at[k % self.N],
            self.ssem.at[i, k % self.N],
            self.rsem.at[i, k % self.N],
            self.cube.devs[i + 1],
        )

    def before_write(self, k):
        @pl.when(k >= self.NSD)
        def _():
            self.core_copy(k - self.NSD).wait_send()

    def push(self, k):
        @pl.when(k >= self.ND)
        def _():
            pl.semaphore_wait(self.credit, 1)

        self.core_copy(k).start()

    def finish(self):
        for k in range(NU - self.NSD, NU):
            self.core_copy(k).wait_send()
        pl.semaphore_wait(self.credit, self.ND)

    def begin(self, k):
        self.core_copy(k).wait_recv()
        self.acc[k % self.NA] = self.acc[k % self.NA] + self.inc[k % self.ND]
        pl.semaphore_signal(self.credit, inc=1, device_id=self.cube.devs[0], device_id_type=MESH)
        self.copy(0, k).start()

    def tick(self, t, final):
        for i in range(4):
            u = t - (i + 1) * self.LAG

            @pl.when((u >= 0) & (u < NU))
            def _(i=i, u=u):
                n = ROWS[i + 1]
                self.copy(i, u).wait()
                rows = pl.ds(aligned(self.cube.keep[i], n), n)
                value = self.acc[u % self.NA, rows, :] + self.recv[i][u % self.N]
                if i < 3:
                    self.acc[u % self.NA, rows, :] = value
                    self.copy(i + 1, u).start()
                else:
                    final(u, value)


class Gather:
    N = 8

    def __init__(self, cube, units, lag, block, ssem, rsem, first=None, local=None):
        self.cube, self.units, self.lag, self.block = cube, units, lag, block
        self.ssem, self.rsem, self.first, self.local = ssem, rsem, first, local

    @classmethod
    def scratch(cls):
        return [DMA((5, cls.N)), DMA((5, cls.N))]

    def copy(self, a, u):
        n = ROWS[4 - a]
        base = 0 if a == 4 else aligned(self.cube.keep[3 - a], n)
        here = self.block(u, pl.ds(base, n))
        src = self.first(u) if a == 0 and self.first is not None else here
        return remote(src, here, self.ssem.at[a, u % self.N], self.rsem.at[a, u % self.N], self.cube.devs[4 - a])

    def tick(self, t):
        for a in range(6):
            u = t - a * self.lag

            @pl.when((u >= 0) & (u < self.units))
            def _(a=a, u=u):
                if a > 0:
                    self.copy(a - 1, u).wait()
                if self.local is not None:
                    if a == 0:
                        self.local(u).start()
                    elif a == 1:
                        self.local(u).wait()
                if a < 5:
                    self.copy(a, u).start()


class Spread:
    def __init__(self, cube, refs):
        self.cube = cube
        self.tiles, self.mine, self.ssem, self.rsem = refs

    @staticmethod
    def scratch():
        return [pltpu.VMEM((DEVICES, 8, 128), f32), pltpu.VMEM((8, 128), f32), DMA((DEVICES,)), DMA((DEVICES,))]

    def copy(self, i, source):
        dev, _ = self.cube.other(i)
        return remote(self.mine, self.tiles.at[source], self.ssem.at[i], self.rsem.at[source], dev)

    def send(self, tile):
        self.mine[...] = tile
        self.tiles[self.cube.me] = tile

        def step(i, carry):
            self.copy(i, self.cube.me).start()
            return carry

        lax.fori_loop(1, DEVICES, step, 0)

    def total(self):
        def step(i, carry):
            _, source = self.cube.other(i)
            self.copy(i, source).wait_recv()
            self.copy(i, self.cube.me).wait_send()
            return carry

        lax.fori_loop(1, DEVICES, step, 0)
        out = self.tiles[0]
        for n in range(1, DEVICES):
            out = out + self.tiles[n]
        return out


def fold(rows):
    out = jnp.zeros((8, 128), f32)
    for r in range(0, rows.shape[0], 8):
        for q in range(0, rows.shape[1], 128):
            out = out + rows[r : r + 8, q : q + 128]
    return out


def dot(a, b, ca=1, cb=0):
    return lax.dot_general(a, b, (((ca,), (cb,)), ((), ())), preferred_element_type=f32)


def step_kernel(
    tokens, x_in, y_in, win, wout, parts, loss_out, hs, us, acts,
    h, u, a, d, wts, g, shard, turn, loss, norm,
    sx, sy, sa, sb, su, sact, sh, so, slocal, gsend, grecv, hsend, hrecv, *refs,
):
    rows = tokens // 2
    cube = Cube()
    scatter = ReduceScatter(cube, refs[:12])
    norm_sum = Spread(cube, refs[12:16])
    loss_sum = Spread(cube, refs[16:20])
    row = cube.keep[3]
    col = cube.core * HALF
    stage = scatter.acc
    inv_count = 1.0 / (tokens * DEVICES * D)
    barrier = pltpu.get_barrier_semaphore()

    def greet(i, carry):
        pl.semaphore_signal(barrier, inc=1, device_id=cube.other(i)[0], device_id_type=MESH)
        return carry

    def copy(src, dst, sem):
        return pltpu.make_async_copy(src, dst, sem)

    def part(r):
        return pl.ds(aligned(r * rows, 16), rows)

    def load_a(l, j):
        return copy(win.at[l, :, pl.ds(aligned(j * W, W), W)], stage.at[j], sa.at[j])

    def load_b(l, j):
        return copy(
            wout.at[l, pl.ds(aligned((j // 2) * 512, 512), 512), pl.ds(aligned((j % 2) * W, W), W)],
            stage.at[8 + j],
            sb.at[j],
        )

    def start_all(load, l):
        def step(j, carry):
            load(l, j).start()
            return carry

        lax.fori_loop(0, 8, step, 0)

    def wait_all(load, l):
        def step(j, carry):
            load(l, j).wait()
            return carry

        lax.fori_loop(0, 8, step, 0)

    def round_a(l, j):
        wts[2 * l, :, pl.ds(aligned(j * W, W), W)] = stage[j].astype(bf16)

    def round_b(l, j):
        block = stage[8 + j].T.astype(bf16)
        wts[2 * l + 1, pl.ds(aligned((j % 2) * W, W), W), pl.ds(aligned((j // 2) * 512, 512), 512)] = block

    def keep_a(l):
        for j in range(4):
            shard[(LAYERS - 1 - l) * 8 + 4 + j] = stage[cube.core * 4 + j, pl.ds(aligned(row, 32), 32), :]

    def keep_b(l):
        for j in range(4):
            slot = 8 + (cube.core * 2 + j // 2) * 2 + row // W
            lanes = pl.ds(aligned(((row % W) // 128) * 128, 128), 128)
            turn[...] = stage[slot, pl.ds((j % 2) * W, W), lanes].T
            shard[(LAYERS - 1 - l) * 8 + j] = turn[pl.ds(aligned(row % 128, 32), 32), :]

    def save_u(l, r):
        return copy(u.at[part(r), :], us.at[l, part(r), :], su.at[r])

    def save_act(l, r):
        return copy(a.at[part(r), :], acts.at[l, part(r), :], sact.at[r])

    def save_h(l):
        return copy(h.at[l % 2], hs.at[l], sh.at[l % 2])

    copy_x = copy(x_in, h.at[0], sx)
    copy_y = copy(y_in, d, sy)

    def forward(tick, before_in, before_out, beside_in, beside_out):
        def layer(l, carry):
            cur = l % 2
            before_in(l)

            def half_in(r, carry):
                @pl.when(l >= 1)
                def _():
                    save_u(l - 1, r).wait()
                    save_act(l - 1, r).wait()

                acc = dot(h[cur, part(r), :], wts[2 * l])
                pre = acc.astype(bf16)
                u[part(r), :] = pre
                a[part(r), :] = gelu(pre.astype(f32)).astype(bf16)
                beside_in(l, r)

                @pl.when(l < LAYERS - 1)
                def _():
                    save_u(l, r).start()
                    save_act(l, r).start()

                tick(4 * l + r)
                return carry

            lax.fori_loop(0, 2, half_in, 0)
            before_out(l)

            @pl.when(l >= 1)
            def _():
                save_h(l - 1).wait()

            def half_out(r, carry):
                acc = dot(a[part(r), :], wts[2 * l + 1], 1, 1)
                h[1 - cur, part(r), :] = (h[cur, part(r), :].astype(f32) + acc).astype(bf16)
                beside_out(l, r)
                tick(4 * l + 2 + r)
                return carry

            lax.fori_loop(0, 2, half_out, 0)

            @pl.when(l < LAYERS - 1)
            def _():
                save_h(l + 1).start()

            return carry

        lax.fori_loop(0, LAYERS, layer, 0)
        save_h(LAYERS - 1).wait()
        copy_y.wait()

    def backward(tick):
        own, away = cube.core * HALF, (1 - cube.core) * HALF

        def load_h(l):
            return copy(hs.at[l], h.at[1], sh.at[1])

        def load_u(l):
            return copy(us.at[l], u, su.at[0])

        def load_act(l):
            return copy(acts.at[l], a, sact.at[0])

        def produce(k, lhs, src, pair):
            scatter.before_write(k)
            scatter.before_write(k + 1)
            value = dot(lhs[...], src[:, pl.ds(aligned(away + pair * 512, 512), 512)], 0, 0)
            scatter.out[k % scatter.NSD] = value[:, :W]
            scatter.out[(k + 1) % scatter.NSD] = value[:, W:]
            scatter.push(k)
            scatter.push(k + 1)
            value = dot(lhs[...], src[:, pl.ds(aligned(own + pair * 512, 512), 512)], 0, 0)
            scatter.acc[k % scatter.NA] = value[:, :W]
            scatter.acc[(k + 1) % scatter.NA] = value[:, W:]

        def begin_pair(k, p):
            @pl.when(p == 1)
            def _():
                scatter.begin(k - 1)

            scatter.begin(k)

        def begin_last(k, r):
            @pl.when(r == 0)
            def _():
                scatter.begin(k)

        def layer(i, carry):
            l = LAYERS - 1 - i
            more = i < LAYERS - 1

            @pl.when(i > 0)
            def _():
                load_act(l).wait()

            def out_pair(p, carry):
                produce(i * 8 + 2 * p, d, a, p)
                begin_pair(i * 8 + 2 * p, p)
                tick(i * 8 + p)
                return carry

            lax.fori_loop(0, 2, out_pair, 0)

            @pl.when(more)
            def _():
                load_act(l - 1).start()

            @pl.when(i > 0)
            def _():
                load_u(l).wait()

            def slope_half(r, carry):
                for n in range(2):
                    cs = slice(n * HALF, (n + 1) * HALF)
                    da = dot(d[part(r), :], wts[2 * l + 1, :, cs])
                    u[part(r), cs] = (da * gelu_slope(u[part(r), cs].astype(f32))).astype(bf16)
                begin_last(i * 8 + 3, r)
                tick(i * 8 + 2 + r)
                return carry

            lax.fori_loop(0, 2, slope_half, 0)

            @pl.when(i > 0)
            def _():
                load_h(l).wait()

            def in_pair(p, carry):
                produce(i * 8 + 4 + 2 * p, h.at[1], u, p)
                begin_pair(i * 8 + 4 + 2 * p, p)
                tick(i * 8 + 4 + p)
                return carry

            lax.fori_loop(0, 2, in_pair, 0)

            @pl.when(more)
            def _():
                load_h(l - 1).start()

            def back_half(r, carry):
                @pl.when(more)
                def _():
                    acc = dot(u[part(r), :], wts[2 * l], 1, 1)
                    d[part(r), :] = (d[part(r), :].astype(f32) + acc).astype(bf16)

                begin_last(i * 8 + 7, r)
                tick(i * 8 + 6 + r)
                return carry

            lax.fori_loop(0, 2, back_half, 0)

            @pl.when(more)
            def _():
                load_u(l - 1).start()

            return carry

        lax.fori_loop(0, LAYERS, layer, 0)

    def nothing(*_):
        pass

    copy_x.start()
    start_all(load_a, 0)
    start_all(load_b, 0)
    copy_y.start()
    lax.fori_loop(1, DEVICES, greet, 0)
    copy_x.wait()
    save_h(0).start()
    wait_all(load_a, 0)

    def round_first(j, carry):
        round_a(0, j)
        return carry

    lax.fori_loop(0, 8, round_first, 0)

    def before_in_1(l):
        @pl.when(l == 0)
        def _():
            keep_a(0)

        wait_all(load_b, l)
        keep_b(l)

        @pl.when(l < LAYERS - 1)
        def _():
            start_all(load_a, l + 1)

    def beside_in_1(l, r):
        for j in range(4):
            round_b(l, r * 4 + j)

    def before_out_1(l):
        @pl.when(l < LAYERS - 1)
        def _():
            start_all(load_b, l + 1)
            wait_all(load_a, l + 1)
            keep_a(l + 1)

    def beside_out_1(l, r):
        for j in range(4):
            round_a(jnp.minimum(l + 1, LAYERS - 1), r * 4 + j)

    forward(nothing, before_in_1, before_out_1, beside_in_1, beside_out_1)
    for r in range(2):
        diff = h[0, part(r), :].astype(f32) - d[part(r), :].astype(f32)
        d[part(r), :] = (diff * inv_count).astype(bf16)
    pl.semaphore_wait(barrier, DEVICES - 1)

    norm[...] = jnp.zeros_like(norm)

    def final_1(unit, value):
        g[unit] = value
        norm[...] += value * value

    def tick_1(t):
        scatter.tick(t, final_1)

    backward(tick_1)

    def rest_1(t, carry):
        tick_1(t)
        return carry

    copy_x.start()
    lax.fori_loop(NU, scatter.TICKS, rest_1, 0)
    norm_sum.send(fold(norm[...]))
    copy_y.start()
    scatter.finish()
    total = norm_sum.total()
    total = jnp.sum(jnp.sum(total, axis=0, keepdims=True), axis=1, keepdims=True)
    scale = (RHO_REL * math.sqrt(LAYERS * F + D)) / jnp.sqrt(total)

    def perturb(m, carry):
        k0 = (LAYERS - 1 - m // 2) * 8 + 4 - (m % 2) * 4
        for j in range(4):
            value = shard[k0 + j] + scale * g[k0 + j]
            wts[m, pl.ds(aligned(row, 32), 32), pl.ds(aligned(col + j * W, W), W)] = value.astype(bf16)
        return carry

    lax.fori_loop(0, 2 * LAYERS, perturb, 0)

    def weight_block(unit, rs):
        return wts.at[unit // 2, rs, pl.ds(aligned(col + (unit % 2) * 512, 512), 512)]

    weights = Gather(cube, 4 * LAYERS, 2, weight_block, gsend, grecv)
    lead = 5 * weights.lag + 2

    def first(t, carry):
        weights.tick(t)
        return carry

    lax.fori_loop(0, lead, first, 0)
    copy_x.wait()
    save_h(0).start()
    forward(lambda t: weights.tick(lead + t), nothing, nothing, nothing, nothing)
    squares = jnp.zeros((1, D), f32)
    for r in range(2):
        diff = h[0, part(r), :].astype(f32) - d[part(r), :].astype(f32)
        d[part(r), :] = (diff * inv_count).astype(bf16)
        squares = squares + jnp.sum(diff * diff, axis=0, keepdims=True)
    lanes = squares[:, :128] + squares[:, 128:256] + squares[:, 256:384] + squares[:, 384:]
    top = lax.broadcasted_iota(jnp.int32, (8, 128), 0) == 0
    loss_sum.send(jnp.where(top, jnp.broadcast_to(lanes, (8, 128)), 0.0))

    late = 4 * scatter.LAG + 1

    def new_block(unit, rs):
        return parts.at[unit, cube.core, rs, :]

    def local(unit):
        return copy(shard.at[unit], new_block(unit, pl.ds(aligned(row, 32), 32)), slocal.at[unit % Gather.N])

    updates = Gather(cube, NU, 2, new_block, hsend, hrecv, lambda unit: shard.at[unit], local)

    def final_2(unit, value):
        shard[unit] = shard[unit] - LEARN_RATE * value

    def tick_2(t):
        scatter.tick(t, final_2)
        updates.tick(t - late)

    backward(tick_2)

    def rest_2(t, carry):
        tick_2(t)
        return carry

    lax.fori_loop(NU, NU + late + 5 * updates.lag, rest_2, 0)
    scatter.finish()
    loss[...] = loss_sum.total()
    save_loss = copy(loss, loss_out, so)
    save_loss.start()
    save_loss.wait()


def place_kernel(tokens, parts, new_in, new_out, straight, before, after, s_load, s_store, t_load, t_store):
    slots, ahead = straight.shape[0], 4

    def where(n):
        return n // 8, (n // 4) % 2, n % 4

    def load_in(n):
        l, c, j = where(n)
        return pltpu.make_async_copy(parts.at[(LAYERS - 1 - l) * 8 + 4 + j, c], straight.at[n % slots], s_load.at[n % slots])

    def store_in(n):
        l, c, j = where(n)
        cols = pl.ds(aligned(c * HALF + j * W, W), W)
        return pltpu.make_async_copy(straight.at[n % slots], new_in.at[l, :, cols], s_store.at[n % slots])

    def load_out(n):
        l, c, j = where(n)
        return pltpu.make_async_copy(parts.at[(LAYERS - 1 - l) * 8 + j, c], before.at[n % slots], t_load.at[n % slots])

    def store_out(n):
        l, c, j = where(n)
        rows = pl.ds(aligned(c * HALF + j * W, W), W)
        return pltpu.make_async_copy(after.at[n % slots], new_out.at[l, rows, :], t_store.at[n % slots])

    for n in range(ahead):
        load_in(n).start()
        load_out(n).start()

    def step(n, carry):
        load_in(n).wait()
        store_in(n).start()

        @pl.when(n >= slots)
        def _():
            store_out(n - slots).wait()

        load_out(n).wait()
        after[n % slots] = before[n % slots].T
        store_out(n).start()

        @pl.when(n + ahead < NU)
        def _():
            @pl.when(n + ahead >= slots)
            def _():
                store_in(n + ahead - slots).wait()

            load_in(n + ahead).start()
            load_out(n + ahead).start()

        return carry

    lax.fori_loop(0, NU, step, 0)
    for n in range(NU - slots, NU):
        store_in(n).wait()
        store_out(n).wait()


def solution(mesh):
    axes = tuple(mesh.axis_names)
    spec = P(axes, None, None)
    S = jax.ShapeDtypeStruct
    VM = pltpu.VMEM

    def step(images, targets, w_in, w_out):
        tokens = images.shape[0] * images.shape[1]
        x = jnp.swapaxes(images, 0, 1).reshape(tokens, D)
        y = jnp.swapaxes(targets, 0, 1).reshape(tokens, D)

        def call(kernel, outs, scratch, *args, collective=None):
            params = dict(vmem_limit_bytes=VMEM_LIMIT)
            if collective is not None:
                params.update(collective_id=collective, has_side_effects=True)
            return pl.pallas_call(
                lambda *refs: kernel(tokens, *refs),
                out_shape=outs,
                in_specs=[ANY] * len(args),
                out_specs=[ANY] * len(outs),
                scratch_shapes=scratch,
                compiler_params=pltpu.CompilerParams(**params),
                name=kernel.__name__,
            )(*args)

        parts, loss, _, _, _ = call(
            step_kernel,
            [S((NU, 2, D, W), f32), S((8, 128), f32), S((LAYERS, tokens, D), bf16)]
            + [S((LAYERS - 1, tokens, F), bf16)] * 2,
            [VM((2, tokens, D), bf16), VM((tokens, F), bf16), VM((tokens, F), bf16), VM((tokens, D), bf16)]
            + [VM((2 * LAYERS, D, F), bf16), VM((NU, 32, W), f32), VM((NU, 32, W), f32), VM((128, W), f32)]
            + [VM((8, 128), f32), VM((32, W), f32)]
            + [DMA, DMA, DMA((8,)), DMA((8,)), DMA((2,)), DMA((2,)), DMA((2,)), DMA, DMA((Gather.N,))]
            + Gather.scratch()
            + Gather.scratch()
            + ReduceScatter.scratch()
            + Spread.scratch()
            + Spread.scratch(),
            x, y, w_in, w_out,
            collective=1,
        )
        new_in, new_out = call(
            place_kernel,
            [S((LAYERS, D, F), f32), S((LAYERS, F, D), f32)],
            [VM((8, D, W), f32), VM((8, D, W), f32), VM((8, W, D), f32)] + [DMA((8,))] * 4,
            parts,
        )
        return new_in, new_out, (0.5 * jnp.sum(loss)) * (1.0 / (tokens * DEVICES * D))

    return jax.shard_map(step, mesh=mesh, in_specs=(spec, spec, P(), P()), out_specs=(P(), P(), P()), check_vma=False)
```

```python
import math

import jax
import jax.numpy as jnp
from jax import lax
from jax.experimental import pallas as pl
from jax.experimental.pallas import tpu as pltpu
from jax.sharding import PartitionSpec as P

MESH = pl.DeviceIdType.MESH
f32 = jnp.float32
bf16 = jnp.bfloat16
RHO_REL = 0.1
LEARN_RATE = 8.0
SQRT_HALF = 0.7071067811865476
INV_SQRT_PI = 0.5641895835477563
LOG2_E = 1.4426950408889634
LAYERS, D, F = 4, 512, 2048
DEVICES = 32
HALF = F // 2
W = 256
NU = 32
ROWS = (512, 256, 128, 64, 32)
VMEM_LIMIT = 62 * 2**20

ANY = pl.BlockSpec(memory_space=pl.ANY)
DMA = pltpu.SemaphoreType.DMA


def aligned(value, multiple):
    return pl.multiple_of(value, multiple)


def gelu(u):
    half = (u * bf16(0.5)).astype(f32)
    return half * (1.0 + lax.erf(half * (2.0 * SQRT_HALF)))


def gelu_slope_twice(x):
    z = x * SQRT_HALF
    return (1.0 + lax.erf(z)) + (z * (2.0 * INV_SQRT_PI)) * jnp.exp2(z * z * (-LOG2_E))


def coords():
    z, y, dd = lax.axis_index("model"), lax.axis_index("sub"), lax.axis_index("data")
    return z, y, dd // 2, dd % 2


class Cube:
    def __init__(self):
        z, y, x, c = coords()
        fx, fy = 1 - 2 * x, 1 - 2 * y
        self.core = c
        self.devs = (
            (z, y, x * 2 + (1 - c)),
            (z, y + c * fy, (x + (1 - c) * fx) * 2 + c),
            (z + 1 - 2 * (z % 2), y, x * 2 + c),
            (z, y + (1 - c) * fy, (x + c * fx) * 2 + c),
            ((z + 2) % 4, y, x * 2 + c),
        )
        bits = (x * (1 - c) + y * c, z % 2, y * (1 - c) + x * c, z // 2)
        self.keep, self.give, base = [], [], 0
        for i in range(4):
            half = ROWS[i + 1]
            self.keep.append(base + bits[i] * half)
            self.give.append(base + (1 - bits[i]) * half)
            base = base + bits[i] * half

        self.me = (z * 2 + y) * 4 + x * 2 + c

    def other(self, i):
        n = lax.rem(self.me + i, DEVICES)
        return (n // 8, (n // 4) % 2, n % 4), n


def remote(src, dst, send_sem, recv_sem, dev):
    return pltpu.make_async_remote_copy(
        src_ref=src, dst_ref=dst, send_sem=send_sem, recv_sem=recv_sem, device_id=dev, device_id_type=MESH
    )


class ReduceScatter:
    NSD, ND, NA, N, LAG = 4, 8, 16, 8, 2
    TICKS = NU + 4 * LAG

    @classmethod
    def scratch(cls):
        n = cls.N
        return [
            pltpu.VMEM((cls.NSD, 512, W), f32),
            pltpu.VMEM((cls.NA, 512, W), f32),
            pltpu.VMEM((cls.ND, 512, W), f32),
            pltpu.VMEM((n, 256, W), f32),
            pltpu.VMEM((n, 128, W), f32),
            pltpu.VMEM((n, 64, W), f32),
            pltpu.VMEM((n, 32, W), f32),
            DMA((cls.NSD,)),
            DMA((cls.ND,)),
            DMA((4, n)),
            DMA((4, n)),
            pltpu.SemaphoreType.REGULAR,
        ]

    def __init__(self, cube, refs):
        self.cube = cube
        (self.out, self.acc, self.inc, r1, r2, r3, r4, self.dsend, self.drecv, self.ssem, self.rsem, self.credit) = refs
        self.recv = (r1, r2, r3, r4)

    def core_copy(self, k):
        return remote(
            self.out.at[k % self.NSD],
            self.inc.at[k % self.ND],
            self.dsend.at[k % self.NSD],
            self.drecv.at[k % self.ND],
            self.cube.devs[0],
        )

    def copy(self, i, k):
        n = ROWS[i + 1]
        return remote(
            self.acc.at[k % self.NA, pl.ds(aligned(self.cube.give[i], n), n), :],
            self.recv[i].at[k % self.N],
            self.ssem.at[i, k % self.N],
            self.rsem.at[i, k % self.N],
            self.cube.devs[i + 1],
        )

    def before_write(self, k):
        @pl.when(k >= self.NSD)
        def _():
            self.core_copy(k - self.NSD).wait_send()

    def push(self, k):
        @pl.when(k >= self.ND)
        def _():
            pl.semaphore_wait(self.credit, 1)

        self.core_copy(k).start()

    def finish(self):
        for k in range(NU - self.NSD, NU):
            self.core_copy(k).wait_send()
        pl.semaphore_wait(self.credit, self.ND)

    def begin(self, k):
        self.core_copy(k).wait_recv()
        self.acc[k % self.NA] = self.acc[k % self.NA] + self.inc[k % self.ND]
        pl.semaphore_signal(self.credit, inc=1, device_id=self.cube.devs[0], device_id_type=MESH)
        self.copy(0, k).start()

    def tick(self, t, final):
        for i in range(4):
            u = t - (i + 1) * self.LAG

            @pl.when((u >= 0) & (u < NU))
            def _(i=i, u=u):
                n = ROWS[i + 1]
                self.copy(i, u).wait()
                rows = pl.ds(aligned(self.cube.keep[i], n), n)
                value = self.acc[u % self.NA, rows, :] + self.recv[i][u % self.N]
                if i < 3:
                    self.acc[u % self.NA, rows, :] = value
                    self.copy(i + 1, u).start()
                else:
                    final(u, value)


class Gather:
    N = 8

    def __init__(self, cube, units, begins, block, ssem, rsem, first=None, local=None):
        self.cube, self.units, self.begins, self.block = cube, units, begins, block
        self.ssem, self.rsem, self.first, self.local = ssem, rsem, first, local

    @classmethod
    def scratch(cls):
        return [DMA((5, cls.N)), DMA((5, cls.N))]

    def copy(self, a, u):
        n = ROWS[4 - a]
        base = 0 if a == 4 else aligned(self.cube.keep[3 - a], n)
        here = self.block(u, pl.ds(base, n))
        src = self.first(u) if a == 0 and self.first is not None else here
        return remote(src, here, self.ssem.at[a, u % self.N], self.rsem.at[a, u % self.N], self.cube.devs[4 - a])

    def tick(self, t):
        for a in range(6):
            u = t - self.begins[a]

            @pl.when((u >= 0) & (u < self.units))
            def _(a=a, u=u):
                if a > 0:
                    self.copy(a - 1, u).wait()
                if self.local is not None:
                    if a == 0:
                        self.local(u).start()
                    elif a == 1:
                        self.local(u).wait()
                if a < 5:
                    self.copy(a, u).start()


class Spread:
    def __init__(self, cube, refs):
        self.cube = cube
        self.tiles, self.mine, self.ssem, self.rsem = refs

    @staticmethod
    def scratch():
        return [pltpu.VMEM((DEVICES, 8, 128), f32), pltpu.VMEM((8, 128), f32), DMA((DEVICES,)), DMA((DEVICES,))]

    def copy(self, i, source):
        dev, _ = self.cube.other(i)
        return remote(self.mine, self.tiles.at[source], self.ssem.at[i], self.rsem.at[source], dev)

    def send(self, tile):
        self.mine[...] = tile
        self.tiles[self.cube.me] = tile

        def step(i, carry):
            self.copy(i, self.cube.me).start()
            return carry

        lax.fori_loop(1, DEVICES, step, 0)

    def total(self):
        def step(i, carry):
            _, source = self.cube.other(i)
            self.copy(i, source).wait_recv()
            self.copy(i, self.cube.me).wait_send()
            return carry

        lax.fori_loop(1, DEVICES, step, 0)
        out = self.tiles[0]
        for n in range(1, DEVICES):
            out = out + self.tiles[n]
        return out


def fold(rows):
    out = jnp.zeros((8, 128), f32)
    for r in range(0, rows.shape[0], 8):
        for q in range(0, rows.shape[1], 128):
            out = out + rows[r : r + 8, q : q + 128]
    return out


def dot(a, b, ca=1, cb=0):
    return lax.dot_general(a, b, (((ca,), (cb,)), ((), ())), preferred_element_type=f32)


def step_kernel(
    tokens, x_in, y_in, win, wout, parts, loss_out, hs, us, acts,
    h, u, a, d, wts, g, shard, turn, loss, norm,
    sx, sy, sa, sb, su, sact, sh, so, slocal, gsend, grecv, hsend, hrecv, *refs,
):
    rows = tokens // 2
    cube = Cube()
    scatter = ReduceScatter(cube, refs[:12])
    norm_sum = Spread(cube, refs[12:16])
    loss_sum = Spread(cube, refs[16:20])
    row = cube.keep[3]
    col = cube.core * HALF
    stage = scatter.acc
    inv_count = 1.0 / (tokens * DEVICES * D)
    barrier = pltpu.get_barrier_semaphore()

    def greet(i, carry):
        pl.semaphore_signal(barrier, inc=1, device_id=cube.other(i)[0], device_id_type=MESH)
        return carry

    def copy(src, dst, sem):
        return pltpu.make_async_copy(src, dst, sem)

    def part(r):
        return pl.ds(aligned(r * rows, 16), rows)

    def load_a(l, j):
        return copy(win.at[l, :, pl.ds(aligned(j * W, W), W)], stage.at[j], sa.at[j])

    def load_b(l, j):
        return copy(
            wout.at[l, pl.ds(aligned((j // 2) * 512, 512), 512), pl.ds(aligned((j % 2) * W, W), W)],
            stage.at[8 + j],
            sb.at[j],
        )

    def start_all(load, l):
        for j in range(8):
            load(l, j).start()

    def wait_all(load, l):
        for j in range(8):
            load(l, j).wait()

    def round_a(l, j):
        wts[2 * l, :, pl.ds(aligned(j * W, W), W)] = stage[j].astype(bf16)

    def round_b(l, j):
        block = stage[8 + j].T.astype(bf16)
        wts[2 * l + 1, pl.ds(aligned((j % 2) * W, W), W), pl.ds(aligned((j // 2) * 512, 512), 512)] = block

    def keep_a(l, j):
        shard[(LAYERS - 1 - l) * 8 + 4 + j] = stage[cube.core * 4 + j, pl.ds(aligned(row, 32), 32), :]

    def keep_b(l, j):
        slot = 8 + (cube.core * 2 + j // 2) * 2 + row // W
        lanes = pl.ds(aligned(((row % W) // 128) * 128, 128), 128)
        turn[j] = stage[slot, pl.ds(aligned((j % 2) * W, W), W), lanes].T
        shard[(LAYERS - 1 - l) * 8 + j] = turn[j, pl.ds(aligned(row % 128, 32), 32), :]

    def save_u(l, r):
        return copy(u.at[part(r), :], us.at[l, part(r), :], su.at[r])

    def save_act(l, r):
        return copy(a.at[part(r), :], acts.at[l, part(r), :], sact.at[r])

    def save_h(l):
        return copy(h.at[l % 2], hs.at[l], sh.at[l % 2])

    copy_x = copy(x_in, h.at[0], sx)
    copy_y = copy(y_in, d, sy)

    def forward(tick, before_in, before_out, beside_in, beside_out, whole):
        def layer(l, carry):
            cur = l % 2

            def wait_saves(r):
                @pl.when(l >= 1)
                def _():
                    save_u(l - 1, r).wait()
                    save_act(l - 1, r).wait()

            def start_saves(r):
                @pl.when(l < LAYERS - 1)
                def _():
                    save_u(l, r).start()
                    save_act(l, r).start()

            def rows_in(r):
                u[part(r), :] = dot(h[cur, part(r), :], wts[2 * l]).astype(bf16)
                a[part(r), :] = gelu(u[part(r), :]).astype(bf16)
                beside_in(l, r)

            def rows_out(r):
                acc = dot(a[part(r), :], wts[2 * l + 1], 1, 1)
                h[1 - cur, part(r), :] = (h[cur, part(r), :].astype(f32) + acc).astype(bf16)
                beside_out(l, r)

            def half_in(r, carry):
                wait_saves(r)
                rows_in(r)
                start_saves(r)
                tick(4 * l + r)
                return carry

            def half_out(r, carry):
                rows_out(r)
                tick(4 * l + 2 + r)
                return carry

            before_in(l)
            if whole:
                for step in (wait_saves, rows_in, start_saves):
                    for r in range(2):
                        step(r)
            else:
                lax.fori_loop(0, 2, half_in, 0)
            before_out(l)

            @pl.when(l >= 1)
            def _():
                save_h(l - 1).wait()

            if whole:
                for r in range(2):
                    rows_out(r)
            else:
                lax.fori_loop(0, 2, half_out, 0)

            @pl.when(l < LAYERS - 1)
            def _():
                save_h(l + 1).start()

            return carry

        lax.fori_loop(0, LAYERS, layer, 0)
        save_h(LAYERS - 1).wait()
        copy_y.wait()

    def backward(tick):
        own, away = cube.core * HALF, (1 - cube.core) * HALF

        def load_h(l):
            return copy(hs.at[l], h.at[1], sh.at[1])

        def load_u(l):
            return copy(us.at[l], u, su.at[0])

        def load_act(l):
            return copy(acts.at[l], a, sact.at[0])

        def produce(k, lhs, src, pair):
            scatter.before_write(k)
            scatter.before_write(k + 1)
            value = dot(lhs[...], src[:, pl.ds(aligned(away + pair * 512, 512), 512)], 0, 0)
            scatter.out[k % scatter.NSD] = value[:, :W]
            scatter.out[(k + 1) % scatter.NSD] = value[:, W:]
            scatter.push(k)
            scatter.push(k + 1)
            value = dot(lhs[...], src[:, pl.ds(aligned(own + pair * 512, 512), 512)], 0, 0)
            scatter.acc[k % scatter.NA] = value[:, :W]
            scatter.acc[(k + 1) % scatter.NA] = value[:, W:]

        def begin_pair(k, p):
            @pl.when(p == 1)
            def _():
                scatter.begin(k - 1)

            scatter.begin(k)

        def begin_last(k, r):
            @pl.when(r == 0)
            def _():
                scatter.begin(k)

        def layer(i, carry):
            l = LAYERS - 1 - i
            more = i < LAYERS - 1

            @pl.when(i > 0)
            def _():
                load_act(l).wait()

            def out_pair(p, carry):
                produce(i * 8 + 2 * p, d, a, p)
                begin_pair(i * 8 + 2 * p, p)
                tick(i * 8 + p)
                return carry

            lax.fori_loop(0, 2, out_pair, 0)

            @pl.when(more)
            def _():
                load_act(l - 1).start()

            @pl.when(i > 0)
            def _():
                load_u(l).wait()

            def slope_half(r, carry):
                half = d[part(r), :] * bf16(0.5)
                for n in range(2):
                    cs = slice(n * HALF, (n + 1) * HALF)
                    da = dot(half, wts[2 * l + 1, :, cs])
                    u[part(r), cs] = (da * gelu_slope_twice(u[part(r), cs].astype(f32))).astype(bf16)
                begin_last(i * 8 + 3, r)
                tick(i * 8 + 2 + r)
                return carry

            lax.fori_loop(0, 2, slope_half, 0)

            @pl.when(i > 0)
            def _():
                load_h(l).wait()

            def in_pair(p, carry):
                produce(i * 8 + 4 + 2 * p, h.at[1], u, p)
                begin_pair(i * 8 + 4 + 2 * p, p)
                tick(i * 8 + 4 + p)
                return carry

            lax.fori_loop(0, 2, in_pair, 0)

            @pl.when(more)
            def _():
                load_h(l - 1).start()

            def back_half(r, carry):
                @pl.when(more)
                def _():
                    acc = dot(u[part(r), :], wts[2 * l], 1, 1)
                    d[part(r), :] = (d[part(r), :].astype(f32) + acc).astype(bf16)

                begin_last(i * 8 + 7, r)
                tick(i * 8 + 6 + r)
                return carry

            lax.fori_loop(0, 2, back_half, 0)

            @pl.when(more)
            def _():
                load_u(l - 1).start()

            return carry

        lax.fori_loop(0, LAYERS, layer, 0)

    def nothing(*_):
        pass

    copy_x.start()
    start_all(load_a, 0)
    start_all(load_b, 0)
    copy_y.start()
    lax.fori_loop(1, DEVICES, greet, 0)
    copy_x.wait()
    save_h(0).start()

    def round_first(j, carry):
        load_a(0, j).wait()
        round_a(0, j)
        return carry

    lax.fori_loop(0, 8, round_first, 0)
    for j in range(4):
        keep_a(0, j)

    def before_in_1(l):
        wait_all(load_b, l)

        @pl.when(l < LAYERS - 1)
        def _():
            start_all(load_a, l + 1)

    def beside_in_1(l, r):
        for j in range(4):
            round_b(l, r * 4 + j)
        for j in range(2):
            keep_b(l, r * 2 + j)

    def before_out_1(l):
        @pl.when(l < LAYERS - 1)
        def _():
            start_all(load_b, l + 1)
            wait_all(load_a, l + 1)

    def beside_out_1(l, r):
        following = jnp.minimum(l + 1, LAYERS - 1)
        for j in range(4):
            round_a(following, r * 4 + j)
        for j in range(2):
            keep_a(following, r * 2 + j)

    forward(nothing, before_in_1, before_out_1, beside_in_1, beside_out_1, False)
    for r in range(2):
        diff = h[0, part(r), :].astype(f32) - d[part(r), :].astype(f32)
        d[part(r), :] = (diff * inv_count).astype(bf16)
    pl.semaphore_wait(barrier, DEVICES - 1)

    norm[...] = jnp.zeros_like(norm)

    def final_1(unit, value):
        g[unit] = value
        norm[...] += value * value

    def tick_1(t):
        scatter.tick(t, final_1)

    backward(tick_1)

    def rest_1(t, carry):
        tick_1(t)
        return carry

    copy_x.start()
    lax.fori_loop(NU, scatter.TICKS, rest_1, 0)
    norm_sum.send(fold(norm[...]))
    copy_y.start()
    scatter.finish()
    total = norm_sum.total()
    total = jnp.sum(jnp.sum(total, axis=0, keepdims=True), axis=1, keepdims=True)
    scale = (RHO_REL * math.sqrt(LAYERS * F + D)) / jnp.sqrt(total)

    def perturb(m, carry):
        k0 = (LAYERS - 1 - m // 2) * 8 + 4 - (m % 2) * 4
        for j in range(4):
            value = shard[k0 + j] + scale * g[k0 + j]
            wts[m, pl.ds(aligned(row, 32), 32), pl.ds(aligned(col + j * W, W), W)] = value.astype(bf16)
        return carry

    lax.fori_loop(0, 2 * LAYERS, perturb, 0)

    def weight_block(unit, rs):
        return wts.at[unit // 2, rs, pl.ds(aligned(col + (unit % 2) * 512, 512), 512)]

    weights = Gather(cube, 4 * LAYERS, (0, 2, 4, 6, 8, 9), weight_block, gsend, grecv)
    lead = weights.begins[5] + 2

    def first(t, carry):
        weights.tick(t)
        return carry

    lax.fori_loop(0, lead, first, 0)
    copy_x.wait()
    save_h(0).start()
    forward(lambda t: weights.tick(lead + t), nothing, nothing, nothing, nothing, False)
    squares = jnp.zeros((1, D), f32)
    for r in range(2):
        diff = h[0, part(r), :].astype(f32) - d[part(r), :].astype(f32)
        d[part(r), :] = (diff * inv_count).astype(bf16)
        squares = squares + jnp.sum(diff * diff, axis=0, keepdims=True)
    lanes = squares[:, :128] + squares[:, 128:256] + squares[:, 256:384] + squares[:, 384:]
    top = lax.broadcasted_iota(jnp.int32, (8, 128), 0) == 0
    loss_sum.send(jnp.where(top, jnp.broadcast_to(lanes, (8, 128)), 0.0))

    late = 4 * scatter.LAG + 1

    def new_block(unit, rs):
        return parts.at[unit, cube.core, rs, :]

    def local(unit):
        return copy(shard.at[unit], new_block(unit, pl.ds(aligned(row, 32), 32)), slocal.at[unit % Gather.N])

    updates = Gather(cube, NU, (0, 2, 4, 6, 8, 10), new_block, hsend, hrecv, lambda unit: shard.at[unit], local)

    def final_2(unit, value):
        shard[unit] = shard[unit] - LEARN_RATE * value

    def tick_2(t):
        scatter.tick(t, final_2)
        updates.tick(t - late)

    backward(tick_2)

    def rest_2(t, carry):
        tick_2(t)
        return carry

    lax.fori_loop(NU, NU + late + updates.begins[5], rest_2, 0)
    scatter.finish()
    loss[...] = loss_sum.total()
    save_loss = copy(loss, loss_out, so)
    save_loss.start()
    save_loss.wait()


def place_kernel(tokens, parts, loss_in, new_in, new_out, loss_out, straight, before, after, loss, s_load, s_store, t_load, t_store, sl):
    slots, ahead = straight.shape[0], 4

    def where(n):
        return n // 8, (n // 4) % 2, n % 4

    def load_in(n):
        l, c, j = where(n)
        return pltpu.make_async_copy(parts.at[(LAYERS - 1 - l) * 8 + 4 + j, c], straight.at[n % slots], s_load.at[n % slots])

    def store_in(n):
        l, c, j = where(n)
        cols = pl.ds(aligned(c * HALF + j * W, W), W)
        return pltpu.make_async_copy(straight.at[n % slots], new_in.at[l, :, cols], s_store.at[n % slots])

    def load_out(n):
        l, c, j = where(n)
        return pltpu.make_async_copy(parts.at[(LAYERS - 1 - l) * 8 + j, c], before.at[n % slots], t_load.at[n % slots])

    def store_out(n):
        l, c, j = where(n)
        rows = pl.ds(aligned(c * HALF + j * W, W), W)
        return pltpu.make_async_copy(after.at[n % slots], new_out.at[l, rows, :], t_store.at[n % slots])

    load_loss = pltpu.make_async_copy(loss_in, loss, sl)
    load_loss.start()
    for n in range(ahead):
        load_in(n).start()
        load_out(n).start()
    load_loss.wait()
    loss_out[0, 0] = (0.5 * jnp.sum(loss[...])) * (1.0 / (tokens * DEVICES * D))

    def step(n, carry):
        load_in(n).wait()
        store_in(n).start()

        @pl.when(n >= slots)
        def _():
            store_out(n - slots).wait()

        load_out(n).wait()
        after[n % slots] = before[n % slots].T
        store_out(n).start()

        @pl.when(n + ahead < NU)
        def _():
            @pl.when(n + ahead >= slots)
            def _():
                store_in(n + ahead - slots).wait()

            load_in(n + ahead).start()
            load_out(n + ahead).start()

        return carry

    lax.fori_loop(0, NU, step, 0)
    for n in range(NU - slots, NU):
        store_in(n).wait()
        store_out(n).wait()


def solution(mesh):
    axes = tuple(mesh.axis_names)
    spec = P(axes, None, None)
    S = jax.ShapeDtypeStruct
    VM = pltpu.VMEM

    def step(images, targets, w_in, w_out):
        tokens = images.shape[0] * images.shape[1]
        x = jnp.swapaxes(images, 0, 1).reshape(tokens, D)
        y = jnp.swapaxes(targets, 0, 1).reshape(tokens, D)

        def call(kernel, outs, scratch, *args, collective=None, out_specs=None):
            params = dict(vmem_limit_bytes=VMEM_LIMIT)
            if collective is not None:
                params.update(collective_id=collective, has_side_effects=True)
            return pl.pallas_call(
                lambda *refs: kernel(tokens, *refs),
                out_shape=outs,
                in_specs=[ANY] * len(args),
                out_specs=out_specs or [ANY] * len(outs),
                scratch_shapes=scratch,
                compiler_params=pltpu.CompilerParams(**params),
                name=kernel.__name__,
            )(*args)

        parts, loss, _, _, _ = call(
            step_kernel,
            [S((NU, 2, D, W), f32), S((8, 128), f32), S((LAYERS, tokens, D), bf16)]
            + [S((LAYERS - 1, tokens, F), bf16)] * 2,
            [VM((2, tokens, D), bf16), VM((tokens, F), bf16), VM((tokens, F), bf16), VM((tokens, D), bf16)]
            + [VM((2 * LAYERS, D, F), bf16), VM((NU, 32, W), f32), VM((NU, 32, W), f32), VM((4, 128, W), f32)]
            + [VM((8, 128), f32), VM((32, W), f32)]
            + [DMA, DMA, DMA((8,)), DMA((8,)), DMA((2,)), DMA((2,)), DMA((2,)), DMA, DMA((Gather.N,))]
            + Gather.scratch()
            + Gather.scratch()
            + ReduceScatter.scratch()
            + Spread.scratch()
            + Spread.scratch(),
            x, y, w_in, w_out,
            collective=1,
        )
        new_in, new_out, mean = call(
            place_kernel,
            [S((LAYERS, D, F), f32), S((LAYERS, F, D), f32), S((1, 1), f32)],
            [VM((8, D, W), f32), VM((8, D, W), f32), VM((8, W, D), f32), VM((8, 128), f32)] + [DMA((8,))] * 4 + [DMA],
            parts, loss,
            out_specs=[ANY, ANY, pl.BlockSpec(memory_space=pltpu.SMEM)],
        )
        return new_in, new_out, mean.reshape(())

    return jax.shard_map(step, mesh=mesh, in_specs=(spec, spec, P(), P()), out_specs=(P(), P(), P()), check_vma=False)
```

```python
import math

import jax
import jax.numpy as jnp
from jax import lax
from jax.experimental import pallas as pl
from jax.experimental.pallas import tpu as pltpu
from jax.sharding import PartitionSpec as P

MESH = pl.DeviceIdType.MESH
f32 = jnp.float32
bf16 = jnp.bfloat16
RHO_REL = 0.1
LEARN_RATE = 8.0
SQRT_HALF = 0.7071067811865476
INV_SQRT_PI = 0.5641895835477563
LOG2_E = 1.4426950408889634
LAYERS, D, F = 4, 512, 2048
DEVICES = 32
HALF = F // 2
W = 256
NU = 32
ROWS = (512, 256, 128, 64, 32)
VMEM_LIMIT = 67_043_328

ANY = pl.BlockSpec(memory_space=pl.ANY)
DMA = pltpu.SemaphoreType.DMA


def aligned(value, multiple):
    return pl.multiple_of(value, multiple)


def gelu(u):
    half = (u * bf16(0.5)).astype(f32)
    return half * (1.0 + lax.erf(half * (2.0 * SQRT_HALF)))


def gelu_slope_twice(x):
    z = x * SQRT_HALF
    return (1.0 + lax.erf(z)) + (z * (2.0 * INV_SQRT_PI)) * jnp.exp2(z * z * (-LOG2_E))


def coords():
    z, y, dd = lax.axis_index("model"), lax.axis_index("sub"), lax.axis_index("data")
    return z, y, dd // 2, dd % 2


class Cube:
    def __init__(self):
        z, y, x, c = coords()
        fx, fy = 1 - 2 * x, 1 - 2 * y
        self.core = c
        self.devs = (
            (z, y, x * 2 + (1 - c)),
            (z, y + c * fy, (x + (1 - c) * fx) * 2 + c),
            (z + 1 - 2 * (z % 2), y, x * 2 + c),
            (z, y + (1 - c) * fy, (x + c * fx) * 2 + c),
            ((z + 2) % 4, y, x * 2 + c),
        )
        bits = (x * (1 - c) + y * c, z % 2, y * (1 - c) + x * c, z // 2)
        self.keep, self.give, base = [], [], 0
        for i in range(4):
            half = ROWS[i + 1]
            self.keep.append(base + bits[i] * half)
            self.give.append(base + (1 - bits[i]) * half)
            base = base + bits[i] * half

        self.me = (z * 2 + y) * 4 + x * 2 + c

    def other(self, i):
        n = lax.rem(self.me + i, DEVICES)
        return (n // 8, (n // 4) % 2, n % 4), n


def remote(src, dst, send_sem, recv_sem, dev):
    return pltpu.make_async_remote_copy(
        src_ref=src, dst_ref=dst, send_sem=send_sem, recv_sem=recv_sem, device_id=dev, device_id_type=MESH
    )


class ReduceScatter:
    NSD, ND, NA, N, LAG = 8, 6, 16, 8, 2
    TICKS = NU + 4 * LAG

    @classmethod
    def scratch(cls):
        n = cls.N
        return [
            pltpu.VMEM((cls.NA + cls.NSD, 512, W), f32),
            pltpu.VMEM((cls.ND, 512, W), f32),
            pltpu.VMEM((n, 256, W), f32),
            pltpu.VMEM((n, 128, W), f32),
            pltpu.VMEM((n, 64, W), f32),
            pltpu.VMEM((n, 32, W), f32),
            DMA((cls.NSD,)),
            DMA((cls.ND,)),
            DMA((4, n)),
            DMA((4, n)),
            pltpu.SemaphoreType.REGULAR,
        ]

    def __init__(self, cube, refs):
        self.cube = cube
        (self.acc, self.inc, r1, r2, r3, r4, self.dsend, self.drecv, self.ssem, self.rsem, self.credit) = refs
        self.recv = (r1, r2, r3, r4)

    def core_copy(self, k):
        return remote(
            self.acc.at[self.NA + k % self.NSD],
            self.inc.at[k % self.ND],
            self.dsend.at[k % self.NSD],
            self.drecv.at[k % self.ND],
            self.cube.devs[0],
        )

    def copy(self, i, k):
        n = ROWS[i + 1]
        return remote(
            self.acc.at[k % self.NA, pl.ds(aligned(self.cube.give[i], n), n), :],
            self.recv[i].at[k % self.N],
            self.ssem.at[i, k % self.N],
            self.rsem.at[i, k % self.N],
            self.cube.devs[i + 1],
        )

    def before_write(self, k):
        @pl.when(k >= self.NSD)
        def _():
            self.core_copy(k - self.NSD).wait_send()

    def push(self, k):
        @pl.when(k >= self.ND)
        def _():
            pl.semaphore_wait(self.credit, 1)

        self.core_copy(k).start()

    def finish(self):
        for k in range(NU - self.NSD, NU):
            self.core_copy(k).wait_send()
        pl.semaphore_wait(self.credit, self.ND)

    def begin(self, k):
        self.core_copy(k).wait_recv()
        self.acc[k % self.NA] = self.acc[k % self.NA] + self.inc[k % self.ND]
        pl.semaphore_signal(self.credit, inc=1, device_id=self.cube.devs[0], device_id_type=MESH)
        self.copy(0, k).start()

    def tick(self, t, final):
        for i in range(4):
            u = t - (i + 1) * self.LAG

            @pl.when((u >= 0) & (u < NU))
            def _(i=i, u=u):
                n = ROWS[i + 1]
                self.copy(i, u).wait()
                rows = pl.ds(aligned(self.cube.keep[i], n), n)
                value = self.acc[u % self.NA, rows, :] + self.recv[i][u % self.N]
                if i < 3:
                    self.acc[u % self.NA, rows, :] = value
                    self.copy(i + 1, u).start()
                else:
                    final(u, value)


class Gather:
    N = 8

    def __init__(self, cube, units, begins, block, ssem, rsem, first=None, local=None):
        self.cube, self.units, self.begins, self.block = cube, units, begins, block
        self.ssem, self.rsem, self.first, self.local = ssem, rsem, first, local

    @classmethod
    def scratch(cls):
        return [DMA((5, cls.N)), DMA((5, cls.N))]

    def copy(self, a, u):
        n = ROWS[4 - a]
        base = 0 if a == 4 else aligned(self.cube.keep[3 - a], n)
        here = self.block(u, pl.ds(base, n))
        src = self.first(u) if a == 0 and self.first is not None else here
        return remote(src, here, self.ssem.at[a, u % self.N], self.rsem.at[a, u % self.N], self.cube.devs[4 - a])

    def tick(self, t):
        for a in range(6):
            u = t - self.begins[a]

            @pl.when((u >= 0) & (u < self.units))
            def _(a=a, u=u):
                if a > 0:
                    self.copy(a - 1, u).wait()
                if self.local is not None:
                    if a == 0:
                        self.local(u).start()
                    elif a == 1:
                        self.local(u).wait()
                if a < 5:
                    self.copy(a, u).start()


class Spread:
    def __init__(self, cube, refs):
        self.cube = cube
        self.tiles, self.mine, self.ssem, self.rsem = refs

    @staticmethod
    def scratch():
        return [pltpu.VMEM((DEVICES, 8, 128), f32), pltpu.VMEM((8, 128), f32), DMA((DEVICES,)), DMA((DEVICES,))]

    def copy(self, i, source):
        dev, _ = self.cube.other(i)
        return remote(self.mine, self.tiles.at[source], self.ssem.at[i], self.rsem.at[source], dev)

    def send(self, tile):
        self.mine[...] = tile
        self.tiles[self.cube.me] = tile

        def step(i, carry):
            self.copy(i, self.cube.me).start()
            return carry

        lax.fori_loop(1, DEVICES, step, 0)

    def total(self):
        def step(i, carry):
            _, source = self.cube.other(i)
            self.copy(i, source).wait_recv()
            self.copy(i, self.cube.me).wait_send()
            return carry

        lax.fori_loop(1, DEVICES, step, 0)
        out = self.tiles[0]
        for n in range(1, DEVICES):
            out = out + self.tiles[n]
        return out


def fold(rows):
    out = jnp.zeros((8, 128), f32)
    for r in range(0, rows.shape[0], 8):
        for q in range(0, rows.shape[1], 128):
            out = out + rows[r : r + 8, q : q + 128]
    return out


def dot(a, b, ca=1, cb=0):
    return lax.dot_general(a, b, (((ca,), (cb,)), ((), ())), preferred_element_type=f32)


def step_kernel(
    tokens, x_in, y_in, win, wout, parts, loss_out, hs, us, acts,
    h, u, a, d, wts, g, shard, turn, loss, norm,
    sx, sy, sa, sb, su, sact, sh, so, slocal, gsend, grecv, hsend, hrecv, *refs,
):
    rows = tokens // 2
    cube = Cube()
    scatter = ReduceScatter(cube, refs[:11])
    norm_sum = Spread(cube, refs[11:15])
    loss_sum = Spread(cube, refs[15:19])
    row = cube.keep[3]
    col = cube.core * HALF
    stage = scatter.acc
    inv_count = 1.0 / (tokens * DEVICES * D)
    barrier = pltpu.get_barrier_semaphore()

    def greet(i, carry):
        pl.semaphore_signal(barrier, inc=1, device_id=cube.other(i)[0], device_id_type=MESH)
        return carry

    def copy(src, dst, sem):
        return pltpu.make_async_copy(src, dst, sem)

    def part(r):
        return pl.ds(aligned(r * rows, 16), rows)

    def slot_a(l, j):
        return (l % 2) * 16 + j

    def load_a(l, j):
        return copy(win.at[l, :, pl.ds(aligned(j * W, W), W)], stage.at[slot_a(l, j)], sa.at[j])

    def load_b(l, j):
        return copy(
            wout.at[l, pl.ds(aligned((j // 2) * 512, 512), 512), pl.ds(aligned((j % 2) * W, W), W)],
            stage.at[8 + j],
            sb.at[j],
        )

    def start_all(load, l):
        for j in range(8):
            load(l, j).start()

    def wait_all(load, l):
        for j in range(8):
            load(l, j).wait()

    def round_a(l, j):
        wts[2 * l, :, pl.ds(aligned(j * W, W), W)] = stage[slot_a(l, j)].astype(bf16)

    def round_b(l, j):
        block = stage[8 + j].T.astype(bf16)
        wts[2 * l + 1, pl.ds(aligned((j % 2) * W, W), W), pl.ds(aligned((j // 2) * 512, 512), 512)] = block

    def keep_a(l, j):
        shard[(LAYERS - 1 - l) * 8 + 4 + j] = stage[slot_a(l, cube.core * 4 + j), pl.ds(aligned(row, 32), 32), :]

    def keep_b(l, j):
        slot = 8 + (cube.core * 2 + j // 2) * 2 + row // W
        lanes = pl.ds(aligned(((row % W) // 128) * 128, 128), 128)
        turn[j] = stage[slot, pl.ds(aligned((j % 2) * W, W), W), lanes].T
        shard[(LAYERS - 1 - l) * 8 + j] = turn[j, pl.ds(aligned(row % 128, 32), 32), :]

    def save_u(l, r):
        return copy(u.at[part(r), :], us.at[l, part(r), :], su.at[r])

    def save_act(l, r):
        return copy(a.at[part(r), :], acts.at[l, part(r), :], sact.at[r])

    def save_h(l):
        return copy(h.at[l % 2], hs.at[l], sh.at[l % 2])

    copy_x = copy(x_in, h.at[0], sx)
    copy_y = copy(y_in, d, sy)

    def forward(tick, before_in, before_out, beside_in):
        def layer(l, carry):
            cur = l % 2

            def half_in(r, carry):
                @pl.when(l >= 1)
                def _():
                    save_u(l - 1, r).wait()

                u[part(r), :] = dot(h[cur, part(r), :], wts[2 * l]).astype(bf16)
                beside_in(l, r)

                @pl.when(l < LAYERS - 1)
                def _():
                    save_u(l, r).start()

                tick(4 * l + r)
                return carry

            def half_out(r, carry):
                @pl.when(l >= 1)
                def _():
                    save_act(l - 1, r).wait()

                a[part(r), :] = gelu(u[part(r), :]).astype(bf16)
                acc = dot(a[part(r), :], wts[2 * l + 1], 1, 1)
                h[1 - cur, part(r), :] = (h[cur, part(r), :].astype(f32) + acc).astype(bf16)

                @pl.when(l < LAYERS - 1)
                def _():
                    save_act(l, r).start()

                tick(4 * l + 2 + r)
                return carry

            before_in(l)
            lax.fori_loop(0, 2, half_in, 0)
            before_out(l)

            @pl.when(l >= 1)
            def _():
                save_h(l - 1).wait()

            lax.fori_loop(0, 2, half_out, 0)

            @pl.when(l < LAYERS - 1)
            def _():
                save_h(l + 1).start()

            return carry

        lax.fori_loop(0, LAYERS, layer, 0)
        save_h(LAYERS - 1).wait()
        copy_y.wait()

    def backward(tick):
        own, away = cube.core * HALF, (1 - cube.core) * HALF

        def load_h(l):
            return copy(hs.at[l], h.at[1], sh.at[1])

        def load_u(l):
            return copy(us.at[l], u, su.at[0])

        def load_act(l):
            return copy(acts.at[l], a, sact.at[0])

        def produce(k, lhs, src, pair):
            scatter.before_write(k)
            scatter.before_write(k + 1)
            value = dot(lhs[...], src[:, pl.ds(aligned(away + pair * 512, 512), 512)], 0, 0)
            scatter.acc[scatter.NA + k % scatter.NSD] = value[:, :W]
            scatter.acc[scatter.NA + (k + 1) % scatter.NSD] = value[:, W:]
            scatter.push(k)
            scatter.push(k + 1)
            value = dot(lhs[...], src[:, pl.ds(aligned(own + pair * 512, 512), 512)], 0, 0)
            scatter.acc[k % scatter.NA] = value[:, :W]
            scatter.acc[(k + 1) % scatter.NA] = value[:, W:]

        def begin_pair(k, p):
            @pl.when(p == 1)
            def _():
                scatter.begin(k - 1)

            scatter.begin(k)

        def begin_last(k, r):
            @pl.when(r == 0)
            def _():
                scatter.begin(k)

        def layer(i, carry):
            l = LAYERS - 1 - i
            more = i < LAYERS - 1

            @pl.when(i > 0)
            def _():
                load_act(l).wait()

            def out_pair(p, carry):
                produce(i * 8 + 2 * p, d, a, p)
                begin_pair(i * 8 + 2 * p, p)
                tick(i * 8 + p)
                return carry

            lax.fori_loop(0, 2, out_pair, 0)

            @pl.when(more)
            def _():
                load_act(l - 1).start()

            @pl.when(i > 0)
            def _():
                load_u(l).wait()

            def slope_half(r, carry):
                half = d[part(r), :] * bf16(0.5)
                for n in range(2):
                    cs = slice(n * HALF, (n + 1) * HALF)
                    da = dot(half, wts[2 * l + 1, :, cs])
                    u[part(r), cs] = (da * gelu_slope_twice(u[part(r), cs].astype(f32))).astype(bf16)
                begin_last(i * 8 + 3, r)
                tick(i * 8 + 2 + r)
                return carry

            lax.fori_loop(0, 2, slope_half, 0)

            @pl.when(i > 0)
            def _():
                load_h(l).wait()

            def in_pair(p, carry):
                produce(i * 8 + 4 + 2 * p, h.at[1], u, p)
                begin_pair(i * 8 + 4 + 2 * p, p)
                tick(i * 8 + 4 + p)
                return carry

            lax.fori_loop(0, 2, in_pair, 0)

            @pl.when(more)
            def _():
                load_h(l - 1).start()

            def back_half(r, carry):
                @pl.when(more)
                def _():
                    acc = dot(u[part(r), :], wts[2 * l], 1, 1)
                    d[part(r), :] = (d[part(r), :].astype(f32) + acc).astype(bf16)

                begin_last(i * 8 + 7, r)
                tick(i * 8 + 6 + r)
                return carry

            lax.fori_loop(0, 2, back_half, 0)

            @pl.when(more)
            def _():
                load_u(l - 1).start()

            return carry

        lax.fori_loop(0, LAYERS, layer, 0)

    def nothing(*_):
        pass

    copy_x.start()
    start_all(load_a, 0)
    start_all(load_b, 0)
    lax.fori_loop(1, DEVICES, greet, 0)
    copy_x.wait()
    save_h(0).start()

    def round_first(j, carry):
        load_a(0, j).wait()
        load_a(1, j).start()
        round_a(0, j)
        return carry

    lax.fori_loop(0, 8, round_first, 0)
    copy_y.start()
    for j in range(4):
        keep_a(0, j)

    def before_in_1(l):
        wait_all(load_b, l)

        @pl.when(l < LAYERS - 1)
        def _():
            wait_all(load_a, l + 1)

        @pl.when(l < LAYERS - 2)
        def _():
            start_all(load_a, l + 2)

    def beside_in_1(l, r):
        following = jnp.minimum(l + 1, LAYERS - 1)
        for j in range(4):
            round_b(l, r * 4 + j)
            round_a(following, r * 4 + j)
        for j in range(2):
            keep_b(l, r * 2 + j)
            keep_a(following, r * 2 + j)

    def before_out_1(l):
        @pl.when(l < LAYERS - 1)
        def _():
            start_all(load_b, l + 1)

    forward(nothing, before_in_1, before_out_1, beside_in_1)
    for r in range(2):
        diff = h[0, part(r), :].astype(f32) - d[part(r), :].astype(f32)
        d[part(r), :] = (diff * inv_count).astype(bf16)
    pl.semaphore_wait(barrier, DEVICES - 1)

    norm[...] = jnp.zeros_like(norm)

    def final_1(unit, value):
        g[unit] = value
        norm[...] += value * value

    def tick_1(t):
        scatter.tick(t, final_1)

    backward(tick_1)

    def rest_1(t, carry):
        tick_1(t)
        return carry

    copy_x.start()
    lax.fori_loop(NU, scatter.TICKS, rest_1, 0)
    norm_sum.send(fold(norm[...]))
    copy_y.start()
    scatter.finish()
    total = norm_sum.total()
    total = jnp.sum(jnp.sum(total, axis=0, keepdims=True), axis=1, keepdims=True)
    scale = (RHO_REL * math.sqrt(LAYERS * F + D)) / jnp.sqrt(total)

    def perturb(m, carry):
        k0 = (LAYERS - 1 - m // 2) * 8 + 4 - (m % 2) * 4
        for j in range(4):
            value = shard[k0 + j] + scale * g[k0 + j]
            wts[m, pl.ds(aligned(row, 32), 32), pl.ds(aligned(col + j * W, W), W)] = value.astype(bf16)
        return carry

    lax.fori_loop(0, 2 * LAYERS, perturb, 0)

    def weight_block(unit, rs):
        return wts.at[unit // 2, rs, pl.ds(aligned(col + (unit % 2) * 512, 512), 512)]

    weights = Gather(cube, 4 * LAYERS, (0, 2, 4, 6, 8, 9), weight_block, gsend, grecv)
    lead = weights.begins[5] + 2

    def first(t, carry):
        weights.tick(t)
        return carry

    lax.fori_loop(0, lead, first, 0)
    copy_x.wait()
    save_h(0).start()
    forward(lambda t: weights.tick(lead + t), nothing, nothing, nothing)
    squares = jnp.zeros((1, D), f32)
    for r in range(2):
        diff = h[0, part(r), :].astype(f32) - d[part(r), :].astype(f32)
        d[part(r), :] = (diff * inv_count).astype(bf16)
        squares = squares + jnp.sum(diff * diff, axis=0, keepdims=True)
    lanes = squares[:, :128] + squares[:, 128:256] + squares[:, 256:384] + squares[:, 384:]
    top = lax.broadcasted_iota(jnp.int32, (8, 128), 0) == 0
    loss_sum.send(jnp.where(top, jnp.broadcast_to(lanes, (8, 128)), 0.0))

    late = 4 * scatter.LAG + 1

    def new_block(unit, rs):
        return parts.at[unit, cube.core, rs, :]

    def local(unit):
        return copy(shard.at[unit], new_block(unit, pl.ds(aligned(row, 32), 32)), slocal.at[unit % Gather.N])

    updates = Gather(cube, NU, (0, 2, 4, 6, 8, 10), new_block, hsend, hrecv, lambda unit: shard.at[unit], local)

    def final_2(unit, value):
        shard[unit] = shard[unit] - LEARN_RATE * value

    def tick_2(t):
        scatter.tick(t, final_2)
        updates.tick(t - late)

    backward(tick_2)

    def rest_2(t, carry):
        tick_2(t)
        return carry

    lax.fori_loop(NU, NU + late + updates.begins[5], rest_2, 0)
    scatter.finish()
    loss[...] = loss_sum.total()
    save_loss = copy(loss, loss_out, so)
    save_loss.start()
    save_loss.wait()


def place_kernel(tokens, parts, loss_in, new_in, new_out, loss_out, straight, before, after, loss, s_load, s_store, t_load, t_store, sl):
    slots, ahead = straight.shape[0], 4

    def where(n):
        return n // 8, (n // 4) % 2, n % 4

    def load_in(n):
        l, c, j = where(n)
        return pltpu.make_async_copy(parts.at[(LAYERS - 1 - l) * 8 + 4 + j, c], straight.at[n % slots], s_load.at[n % slots])

    def store_in(n):
        l, c, j = where(n)
        cols = pl.ds(aligned(c * HALF + j * W, W), W)
        return pltpu.make_async_copy(straight.at[n % slots], new_in.at[l, :, cols], s_store.at[n % slots])

    def load_out(n):
        l, c, j = where(n)
        return pltpu.make_async_copy(parts.at[(LAYERS - 1 - l) * 8 + j, c], before.at[n % slots], t_load.at[n % slots])

    def store_out(n):
        l, c, j = where(n)
        rows = pl.ds(aligned(c * HALF + j * W, W), W)
        return pltpu.make_async_copy(after.at[n % slots], new_out.at[l, rows, :], t_store.at[n % slots])

    load_loss = pltpu.make_async_copy(loss_in, loss, sl)
    load_loss.start()
    for n in range(ahead):
        load_in(n).start()
        load_out(n).start()
    load_loss.wait()
    loss_out[0, 0] = (0.5 * jnp.sum(loss[...])) * (1.0 / (tokens * DEVICES * D))

    def step(n, carry):
        load_in(n).wait()
        store_in(n).start()

        @pl.when(n >= slots)
        def _():
            store_out(n - slots).wait()

        load_out(n).wait()
        after[n % slots] = before[n % slots].T
        store_out(n).start()

        @pl.when(n + ahead < NU)
        def _():
            @pl.when(n + ahead >= slots)
            def _():
                store_in(n + ahead - slots).wait()

            load_in(n + ahead).start()
            load_out(n + ahead).start()

        return carry

    lax.fori_loop(0, NU, step, 0)
    for n in range(NU - slots, NU):
        store_in(n).wait()
        store_out(n).wait()


def solution(mesh):
    axes = tuple(mesh.axis_names)
    spec = P(axes, None, None)
    S = jax.ShapeDtypeStruct
    VM = pltpu.VMEM

    def step(images, targets, w_in, w_out):
        tokens = images.shape[0] * images.shape[1]
        x = jnp.swapaxes(images, 0, 1).reshape(tokens, D)
        y = jnp.swapaxes(targets, 0, 1).reshape(tokens, D)

        def call(kernel, outs, scratch, *args, collective=None, out_specs=None):
            params = dict(vmem_limit_bytes=VMEM_LIMIT)
            if collective is not None:
                params.update(collective_id=collective, has_side_effects=True)
            return pl.pallas_call(
                lambda *refs: kernel(tokens, *refs),
                out_shape=outs,
                in_specs=[ANY] * len(args),
                out_specs=out_specs or [ANY] * len(outs),
                scratch_shapes=scratch,
                compiler_params=pltpu.CompilerParams(**params),
                name=kernel.__name__,
            )(*args)

        parts, loss, _, _, _ = call(
            step_kernel,
            [S((NU, 2, D, W), f32), S((8, 128), f32), S((LAYERS, tokens, D), bf16)]
            + [S((LAYERS - 1, tokens, F), bf16)] * 2,
            [VM((2, tokens, D), bf16), VM((tokens, F), bf16), VM((tokens, F), bf16), VM((tokens, D), bf16)]
            + [VM((2 * LAYERS, D, F), bf16), VM((NU, 32, W), f32), VM((NU, 32, W), f32), VM((4, 128, W), f32)]
            + [VM((8, 128), f32), VM((32, W), f32)]
            + [DMA, DMA, DMA((8,)), DMA((8,)), DMA((2,)), DMA((2,)), DMA((2,)), DMA, DMA((Gather.N,))]
            + Gather.scratch()
            + Gather.scratch()
            + ReduceScatter.scratch()
            + Spread.scratch()
            + Spread.scratch(),
            x, y, w_in, w_out,
            collective=1,
        )
        new_in, new_out, mean = call(
            place_kernel,
            [S((LAYERS, D, F), f32), S((LAYERS, F, D), f32), S((1, 1), f32)],
            [VM((8, D, W), f32), VM((8, D, W), f32), VM((8, W, D), f32), VM((8, 128), f32)] + [DMA((8,))] * 4 + [DMA],
            parts, loss,
            out_specs=[ANY, ANY, pl.BlockSpec(memory_space=pltpu.SMEM)],
        )
        return new_in, new_out, mean.reshape(())

    return jax.shard_map(step, mesh=mesh, in_specs=(spec, spec, P(), P()), out_specs=(P(), P(), P()), check_vma=False)
```
